512 devices in a mesh: expert: 8 (over y, core), dp: 16 (over z), tensor: 4 (over x).
Axes of the slice: x: 4, y: 4, z: 16, core: 2. Of those that a mesh axis runs over, the one named last changes fastest.
Arguments:
- tokens: bfloat16 [2048, 4096], P(('expert', 'dp')), may hold values from -6 to 6
- expert_ids: int32 [2048, 2], P(('expert', 'dp')), may hold values from 0 to 7, all different within a row; in each aligned block of 16 rows (0 to 15, 16 to 31, ...) at most 6 rows name the same one
- route_weight: float32 [2048, 2], P(('expert', 'dp')), may hold values from 0.2 to 1
- gate_weight: bfloat16 [8, 4096, 8192], P('expert', None, ('dp', 'tensor')), may hold values from -0.09375 to 0.09375
- up_weight: bfloat16 [8, 4096, 8192], P('expert', None, ('dp', 'tensor')), may hold values from -0.09375 to 0.09375
- down_weight: bfloat16 [8, 8192, 4096], P('expert', 'dp', 'tensor'), may hold values from -0.125 to 0.125
- past_layers: bfloat16 [8, 2048, 4096], P(None, ('expert', 'dp'), 'tensor'), may hold values from -6 to 6
- dwa_weight: float32 [9], replicated, may hold values from 0.3 to 1.2
Outputs:
- mixed: bfloat16 [2048, 4096], P(('expert', 'dp'), 'tensor')
The draws below stay inside these ranges and needn't reach their ends.
Inputs may be any that keep to these rules, and one draw needn't show every extreme that they name: `expert_ids`: each row names 2 different experts. In each aligned block of 16 rows (the rows of one device) no expert is named more than 6 times; in some blocks one expert is named exactly 6 times.
All inputs are finite; a program needn't handle non-finite values.
Results may differ from the reference program's by a relative error of at most 0.009.
Values may be sent and summed in bfloat16 or wider, within the bound.
No kernel may reach another device: no remote copies, remote signals or barrier semaphores. Data moves between devices by JAX's collectives and lax.ppermute only.
A program may use at most 64 MiB of HBM per device.

```python
import math
import jax
import jax.numpy as jnp
import numpy as np
from jax import lax

D = 4096
FF = 8192
TOP = 2
PAST = 8
TOK_DEV = 16
EXPERTS = 8
CAP = 6
TOKENS = 2048


def levels(key, shape, split, smallest, high):
    def one(axis_at, shards_of):
        steps = jax.random.uniform(jax.random.fold_in(jax.random.fold_in(key, 6), axis_at), (shards_of,), jnp.float32, smallest / len(split), high / len(split))
        return jnp.repeat(jnp.exp(steps), shape[axis_at] // shards_of).reshape((-1,) + (1,) * (len(shape) - axis_at - 1))

    gain = one(*split[0])
    for cut in split[1:]:
        gain = gain * one(*cut)
    return gain


def assign_block(key, own, number, rows, count, top, most, slope):
    ranking = jax.random.permutation(key, count)
    packed, usual = load_shares(count, rows * top, most, slope, True), load_shares(count, rows * top, most, slope, False)
    places = jnp.arange(count)

    def named(tallies, offset_by):
        used = int((tallies > 0).sum())
        fixed = max(1, used // 4)
        shifted = fixed + (places - fixed + offset_by * (used - fixed)) % max(1, count - fixed)
        return jnp.zeros((count,), jnp.int32).at[ranking[jnp.where(places < fixed, places, shifted)]].set(jnp.asarray(tallies, jnp.int32))

    tallies = jnp.where(number % 4 == 0, named(packed, number // 4), named(usual, number - number // 4 - 1))
    mixed = jax.random.permutation(jax.random.fold_in(own, 3), count)
    giver, receiver = mixed[0:count // 2 * 2:2], mixed[1:count // 2 * 2:2]
    margin = jnp.minimum(tallies[giver] - 1, most - tallies[receiver]) // 2
    margin = jnp.where((giver == ranking[0]) | (receiver == ranking[0]) | (tallies[receiver] == 0), 0, jnp.maximum(margin, 0))
    shifted = jax.random.randint(jax.random.fold_in(own, 4), (count // 2,), 0, 1 << 20) % (margin + 1)
    tallies = tallies.at[giver].add(-shifted).at[receiver].add(shifted)
    items = jnp.searchsorted(jnp.cumsum(tallies), jnp.arange(rows * top), side="right").astype(jnp.int32)
    listing = items.reshape(top, rows).T
    listing = listing[jax.random.permutation(jax.random.fold_in(own, 1), rows)]
    offset_by = jax.random.randint(jax.random.fold_in(own, 2), (rows, 1), 0, top)
    return jnp.take_along_axis(listing, (jnp.arange(top)[None, :] + offset_by) % top, axis=1)


def load_shares(amount, total, limit, skew, full):
    loads = [(1 << 20) // math.isqrt(rank ** skew) + 1 for rank in range(1, amount + 1)]
    largest = limit if full else min(limit, max(-(-total // amount), total * loads[0] // sum(loads)))
    least = 1 if total - largest >= amount - 1 else 0
    counts, surplus = [largest] + [least] * (amount - 1), total - largest - least * (amount - 1)
    while surplus > 0:
        movable = [i for i in range(1, amount) if counts[i] < largest] or [i for i in range(1, amount) if counts[i] < limit]
        whole, budget = sum([loads[i] for i in movable]), surplus
        for i in movable:
            extra = min(limit - counts[i], max(1, budget * loads[i] // whole), surplus)
            counts[i] = counts[i] + extra
            surplus = surplus - extra
    return np.array(counts)


def bell_draw(own_key, dims, spread, limit, cuts=(), kind=jnp.bfloat16):
    array = jax.random.normal(own_key, dims, jnp.float32) * spread
    if len(cuts) > 0:
        array = levels(own_key, dims, cuts, -0.22, 0.18) * array
    return jnp.clip(array, min=-limit, max=limit).astype(kind)


def setup_inputs(seed: int = 0) -> dict:
    splits = jax.random.split(jax.random.key(seed), 9)
    tokens = bell_draw(splits[0], (TOKENS, D), 1.0, 6.0, ((0, 128),))
    expert_ids_keys = jax.random.split(jax.random.fold_in(splits[1], 1), TOKENS // TOK_DEV)
    expert_ids_turns = jax.random.permutation(jax.random.fold_in(splits[1], 3), TOKENS // TOK_DEV)
    expert_ids = jax.vmap(lambda own, number: assign_block(jax.random.fold_in(splits[1], 2), own, number, TOK_DEV, EXPERTS, TOP, CAP, 2))(expert_ids_keys, expert_ids_turns).reshape((TOKENS, TOP))
    route_weight = jnp.clip(0.2 + 0.8 * jax.random.uniform(splits[2], (TOKENS, TOP), jnp.float32) ** levels(splits[2], (TOKENS, TOP), ((0, 128),), -0.2, 0.2), 0.2, 1.0)
    gate_weight = bell_draw(splits[3], (EXPERTS, D, FF), D ** -0.5, 0.09375, ((0, 8), (2, 64)))
    up_weight = bell_draw(splits[4], (EXPERTS, D, FF), D ** -0.5, 0.09375, ((0, 8), (2, 64)))
    down_weight = bell_draw(splits[5], (EXPERTS, FF, D), (FF // 4) ** -0.5, 0.125, ((0, 8), (1, 16), (2, 4)))
    past_layers = bell_draw(splits[6], (PAST, TOKENS, D), 1.0, 6.0, ((1, 128), (2, 4)))
    dwa_weight = jnp.clip(jax.random.uniform(splits[7], (PAST + 1,), jnp.float32, 0.3, 1.2), 0.3, 1.2)
    return dict(tokens=tokens, expert_ids=expert_ids, route_weight=route_weight, gate_weight=gate_weight, up_weight=up_weight, down_weight=down_weight, past_layers=past_layers, dwa_weight=dwa_weight)


def expert_slots(expert_ids):
    shards = TOKENS // TOK_DEV
    flat_ids = expert_ids.reshape(shards, TOK_DEV * TOP).astype(jnp.int32)
    matches = (flat_ids[:, :, None] == jnp.arange(EXPERTS, dtype=jnp.int32)[None, None, :]).astype(jnp.int32)
    earlier = jnp.cumsum(matches, axis=1) - matches
    slot_ids = jnp.sum(earlier * matches, axis=2).astype(jnp.int32)
    positions = jnp.arange(shards, dtype=jnp.int32)[:, None] * CAP + slot_ids
    return flat_ids, positions


def reference(tokens, expert_ids, route_weight, gate_weight, up_weight, down_weight, past_layers, dwa_weight):
    shards = TOKENS // TOK_DEV
    buffer_rows = shards * CAP
    flat_ids, positions = expert_slots(expert_ids)
    sources = jnp.repeat(jnp.arange(TOKENS, dtype=jnp.int32).reshape(shards, TOK_DEV), TOP, axis=1)

    def run_expert(inputs):
        number, w_gate, w_up, w_down = inputs
        targets = jnp.where(flat_ids == number, positions, buffer_rows).reshape(-1).astype(jnp.int32)
        picked = jnp.zeros((buffer_rows + 1,), jnp.int32).at[targets].set(sources.reshape(-1))
        rows = tokens[picked[:buffer_rows]]
        gate = jnp.dot(rows, w_gate, preferred_element_type=jnp.float32)
        up = jnp.dot(rows, w_up, preferred_element_type=jnp.float32)
        hidden = (jax.nn.silu(gate) * up).astype(jnp.bfloat16)
        return jnp.dot(hidden, w_down, preferred_element_type=jnp.float32).astype(jnp.bfloat16)

    outputs = lax.map(run_expert, (jnp.arange(EXPERTS, dtype=jnp.int32), gate_weight, up_weight, down_weight))
    index = (flat_ids * buffer_rows + positions).reshape(-1).astype(jnp.int32)
    fetched = outputs.reshape(EXPERTS * buffer_rows, D)[index].astype(jnp.float32).reshape(TOKENS, TOP, D)
    shares = route_weight / jnp.sum(route_weight, axis=1, keepdims=True)
    current = tokens.astype(jnp.float32) + jnp.sum(fetched * shares[:, :, None], axis=1)
    history = jnp.einsum("j,jtd->td", dwa_weight[:PAST].astype(jnp.float32), past_layers.astype(jnp.float32))
    return (dwa_weight[PAST] * current + history).astype(jnp.bfloat16)
```

```python
import jax
import jax.numpy as jnp
from jax import lax
from jax.sharding import PartitionSpec as P


def from_everyone(shard, axis):
    count = lax.axis_size(axis)
    return lax.all_to_all(
        jnp.broadcast_to(shard[None], (count, *shard.shape)), axis, 0, 0, tiled=True
    )


def joined_along(tiles, dim):
    dims = list(tiles.shape[1:])
    dims[dim] *= tiles.shape[0]
    return jnp.moveaxis(tiles, 0, dim).reshape(dims)


def gathered_copies(shard, axis, dim):
    tiles = from_everyone(shard, axis)
    return joined_along(tiles, dim)


def assignment_slots(expert_ids, experts, capacity):
    flat_ids = expert_ids.reshape(-1)
    matches = (flat_ids[:, None] == jnp.arange(experts, dtype=jnp.int32)[None, :]).astype(jnp.int32)
    earlier = jnp.cumsum(matches, axis=0) - matches
    slot_ids = jnp.sum(earlier * matches, axis=1)
    return flat_ids * capacity + slot_ids


def selector(expert_ids, experts, capacity):
    targets = assignment_slots(expert_ids, experts, capacity)
    matched = targets[None, :] == jnp.arange(experts * capacity, dtype=jnp.int32)[:, None]
    chosen = matched.reshape(experts * capacity, expert_ids.shape[0], expert_ids.shape[1])
    return jnp.sum(chosen.astype(jnp.float32), axis=2).astype(jnp.bfloat16)


def per_device(
    tokens, expert_ids, route_weight, gate_weight, up_weight, down_weight, past_layers, dwa_weight
):
    experts = lax.axis_size("expert")
    tok_rows, feature_width = tokens.shape
    chosen_count = expert_ids.shape[1]
    capacity = min(tok_rows, 3 * chosen_count * tok_rows // (2 * experts))
    w_gate = gate_weight[0]
    w_up = up_weight[0]
    w_down = down_weight[0]
    targets = assignment_slots(expert_ids, experts, capacity)
    selected = selector(expert_ids, experts, capacity)
    quarter = w_down.shape[1]
    first_column = lax.axis_index("tensor") * quarter
    own_columns = lax.dynamic_slice_in_dim(tokens, first_column, quarter, 1)
    packed = jnp.dot(selected, own_columns, preferred_element_type=jnp.float32).astype(jnp.bfloat16)
    packed = packed.reshape(experts, capacity, quarter)
    arrived = lax.all_to_all(packed, "expert", split_axis=0, concat_axis=0, tiled=True)
    parts = lax.axis_size("tensor")
    block_rows = lax.all_gather(
        arrived.reshape(experts * capacity, quarter), ("tensor", "dp"), axis=0, tiled=True
    ).reshape(parts, -1, quarter)
    gate = up = 0.0
    for part in range(parts):
        rows = slice(part * quarter, (part + 1) * quarter)
        gate += jnp.dot(block_rows[part], w_gate[rows], preferred_element_type=jnp.float32)
        up += jnp.dot(block_rows[part], w_up[rows], preferred_element_type=jnp.float32)
    hidden = (jax.nn.silu(gate) * up).astype(jnp.bfloat16)
    hidden_wide = gathered_copies(hidden, "tensor", 1)
    expert_out = lax.psum_scatter(
        jnp.dot(hidden_wide, w_down, preferred_element_type=jnp.float32).astype(jnp.bfloat16),
        "dp",
        scatter_dimension=0,
        tiled=True,
    )
    returned_rows = lax.all_to_all(
        expert_out.reshape(experts, capacity, quarter),
        "expert",
        split_axis=0,
        concat_axis=0,
        tiled=True,
    )
    returned_rows = returned_rows.reshape(experts * capacity, quarter)
    fetched = returned_rows[targets].astype(jnp.float32).reshape(tok_rows, chosen_count, quarter)
    shares = route_weight / jnp.sum(route_weight, axis=1, keepdims=True)
    expert_mix = jnp.sum(fetched * shares[:, :, None], axis=1)
    residual = own_columns.astype(jnp.float32)
    current = residual + expert_mix
    depth = past_layers.shape[0]
    history = jnp.einsum("j,jtd->td", dwa_weight[:depth], past_layers.astype(jnp.float32))
    return (dwa_weight[depth] * current + history).astype(jnp.bfloat16)


def solution(mesh):
    return jax.shard_map(
        per_device,
        mesh=mesh,
        in_specs=(
            P(("expert", "dp"), None),
            P(("expert", "dp"), None),
            P(("expert", "dp"), None),
            P("expert", None, ("dp", "tensor")),
            P("expert", None, ("dp", "tensor")),
            P("expert", "dp", "tensor"),
            P(None, ("expert", "dp"), "tensor"),
            P(),
        ),
        out_specs=P(("expert", "dp"), "tensor"),
        check_vma=False,
    )
```

```python
import jax
import jax.numpy as jnp
from jax import lax
from jax.experimental import pallas as pl
from jax.experimental.pallas import tpu as pltpu
from jax.sharding import PartitionSpec as P

RADIX = 4


VMEM = pl.BlockSpec(memory_space=pltpu.VMEM)


def far_groups(count):
    stride = count // RADIX
    return [[low + stride * high for high in range(RADIX)] for low in range(stride)]


def shifted(shard, even_shift, odd_shift):
    experts, count = lax.axis_size("expert"), lax.axis_size("dp")
    pairs = []
    for expert in range(experts):
        shift = odd_shift if expert % 2 else even_shift
        for place in range(count):
            pairs.append((expert * count + place, expert * count + (place + shift) % count))
    return lax.ppermute(shard, ("expert", "dp"), pairs)


def from_neighbours(shard):
    return [shifted(shard, 1, 1), shifted(shard, -1, -1), shifted(shard, 2, -2)]


def to_neighbours(shards):
    below, above, second = shards
    return [shifted(below, -1, -1), shifted(above, 1, 1), shifted(second, -2, 2)]


def assignment_slots(expert_ids, experts, capacity):
    flat_ids = expert_ids.reshape(-1)
    matches = (flat_ids[:, None] == jnp.arange(experts, dtype=jnp.int32)[None, :]).astype(jnp.int32)
    earlier = jnp.cumsum(matches, axis=0) - matches
    slot_ids = jnp.sum(earlier * matches, axis=1)
    return flat_ids * capacity + slot_ids


def selector(targets, shape, rows):
    matched = targets[None, :] == jnp.arange(rows, dtype=jnp.int32)[:, None]
    chosen = matched.reshape(rows, *shape)
    return jnp.sum(chosen.astype(jnp.float32), axis=2).astype(jnp.bfloat16)


def gate_up_parts(sets, weights):
    parts, _, width = weights.shape
    set_rows = sets[0].shape[0]
    rows = set_rows * len(sets)

    def kernel(*refs):
        set_refs, (w_ref, out_ref) = refs[: len(sets)], refs[len(sets) :]
        stacked = jnp.concatenate([ref[...] for ref in set_refs], axis=0)
        for part in range(parts):
            out_ref[part] = jnp.dot(stacked, w_ref[part], preferred_element_type=jnp.float32).astype(out_ref.dtype)

    return pl.pallas_call(
        kernel,
        out_shape=jax.ShapeDtypeStruct((parts, rows, width), jnp.bfloat16),
        in_specs=[VMEM] * (len(sets) + 1),
        out_specs=VMEM,
        name="gate_up_parts",
    )(*sets, weights)


def hidden_copies(parts):
    count, rows, both = parts.shape
    width = both // 2

    def kernel(in_ref, out_ref):
        total = in_ref[0].astype(jnp.float32)
        for part in range(1, count):
            total += in_ref[part].astype(jnp.float32)
        gate, up = total[:, :width], total[:, width:]
        hidden = (gate / (1.0 + jnp.exp(-gate)) * up).astype(out_ref.dtype)
        for part in range(count):
            out_ref[part] = hidden

    return pl.pallas_call(
        kernel,
        out_shape=jax.ShapeDtypeStruct((count, rows, width), jnp.bfloat16),
        in_specs=[VMEM],
        out_specs=VMEM,
        name="hidden_copies",
    )(parts)


def down_sets(hidden, w_down, count):
    parts, rows, _ = hidden.shape
    set_rows = rows // count
    features = w_down.shape[1]

    def kernel(hidden_ref, w_ref, *out_refs):
        wide = jnp.concatenate([hidden_ref[part] for part in range(parts)], axis=1)
        out = jnp.dot(wide, w_ref[...], preferred_element_type=jnp.float32)
        for place, ref in enumerate(out_refs):
            ref[...] = out[place * set_rows : (place + 1) * set_rows].astype(ref.dtype)

    return pl.pallas_call(
        kernel,
        out_shape=[
            jax.ShapeDtypeStruct((set_rows, features), jnp.bfloat16 if place else jnp.float32)
            for place in range(count)
        ],
        in_specs=[VMEM, VMEM],
        out_specs=[VMEM] * count,
        name="down_sets",
    )(hidden, w_down)


def per_device(
    tokens, expert_ids, route_weight, gate_weight, up_weight, down_weight, past_layers, dwa_weight
):
    experts = lax.axis_size("expert")
    parts = lax.axis_size("tensor")
    tok_rows, feature_width = tokens.shape
    chosen_count = expert_ids.shape[1]
    capacity = min(tok_rows, 3 * chosen_count * tok_rows // (2 * experts))
    quarter = feature_width // parts
    groups = far_groups(lax.axis_size("dp"))
    block = experts * capacity

    slabs = [w.reshape(parts, quarter, -1) for w in (gate_weight, up_weight)]
    w_both = lax.all_to_all(jnp.concatenate(slabs, axis=2), "tensor", 0, 0, tiled=True)

    targets = assignment_slots(expert_ids, experts, capacity)
    selected = selector(targets, expert_ids.shape, block)
    first_column = lax.axis_index("tensor") * quarter
    own_columns = lax.dynamic_slice_in_dim(tokens, first_column, quarter, 1)
    packed = jnp.dot(selected, own_columns, preferred_element_type=jnp.float32).astype(jnp.bfloat16)
    arrived = lax.all_to_all(packed.reshape(experts, capacity, quarter), "expert", 0, 0, tiled=True)
    far = lax.all_to_all(
        jnp.broadcast_to(arrived.reshape(1, block, quarter), (RADIX, block, quarter)),
        "dp",
        0,
        0,
        tiled=True,
        axis_index_groups=groups,
    ).reshape(RADIX * block, quarter)
    sets = [far, *from_neighbours(far)]

    partial = gate_up_parts(sets, w_both)
    partial = lax.all_to_all(partial, "tensor", 0, 0, tiled=True)
    hidden = lax.all_to_all(hidden_copies(partial), "tensor", 0, 0, tiled=True)
    own, *others = down_sets(hidden, down_weight[0], len(sets))
    for other in to_neighbours(others):
        own = own + other.astype(jnp.float32)
    own = own.astype(jnp.bfloat16).reshape(RADIX, block, quarter)
    own = lax.all_to_all(own, "dp", 0, 0, tiled=True, axis_index_groups=groups)
    expert_out = jnp.sum(own.astype(jnp.float32), axis=0).astype(jnp.bfloat16)
    returned_rows = lax.all_to_all(
        expert_out.reshape(experts, capacity, quarter), "expert", 0, 0, tiled=True
    ).reshape(block, quarter)

    fetched = returned_rows[targets].astype(jnp.float32).reshape(tok_rows, chosen_count, quarter)
    shares = route_weight / jnp.sum(route_weight, axis=1, keepdims=True)
    expert_mix = jnp.sum(fetched * shares[:, :, None], axis=1)
    current = own_columns.astype(jnp.float32) + expert_mix
    depth = past_layers.shape[0]
    history = jnp.einsum("j,jtd->td", dwa_weight[:depth], past_layers.astype(jnp.float32))
    return (dwa_weight[depth] * current + history).astype(jnp.bfloat16)


def solution(mesh):
    return jax.shard_map(
        per_device,
        mesh=mesh,
        in_specs=(
            P(("expert", "dp"), None),
            P(("expert", "dp"), None),
            P(("expert", "dp"), None),
            P("expert", None, ("dp", "tensor")),
            P("expert", None, ("dp", "tensor")),
            P("expert", "dp", "tensor"),
            P(None, ("expert", "dp"), "tensor"),
            P(),
        ),
        out_specs=P(("expert", "dp"), "tensor"),
        check_vma=False,
    )
```

```python
import jax
import jax.numpy as jnp
from jax import lax
from jax.experimental import pallas as pl
from jax.experimental.pallas import tpu as pltpu
from jax.sharding import PartitionSpec as P

RADIX = 4


LIMIT = pltpu.CompilerParams(vmem_limit_bytes=16 * 2**20)
VMEM = pl.BlockSpec(memory_space=pltpu.VMEM)


def far_groups(count):
    stride = count // RADIX
    return [[low + stride * high for high in range(RADIX)] for low in range(stride)]


def shifted(shard, even_shift, odd_shift):
    experts, count = lax.axis_size("expert"), lax.axis_size("dp")
    pairs = []
    for expert in range(experts):
        shift = odd_shift if expert % 2 else even_shift
        for place in range(count):
            pairs.append((expert * count + place, expert * count + (place + shift) % count))
    return lax.ppermute(shard, ("expert", "dp"), pairs)


def from_neighbours(shard):
    return [shifted(shard, 1, 1), shifted(shard, -1, -1), shifted(shard, 2, -2)]


def to_neighbours(shards):
    below, above, second = shards
    return [shifted(below, -1, -1), shifted(above, 1, 1), shifted(second, -2, 2)]


def assignment_slots(expert_ids, experts, capacity):
    flat_ids = expert_ids.reshape(-1)
    matches = (flat_ids[:, None] == jnp.arange(experts, dtype=jnp.int32)[None, :]).astype(jnp.int32)
    earlier = jnp.cumsum(matches, axis=0) - matches
    slot_ids = jnp.sum(earlier * matches, axis=1)
    return flat_ids * capacity + slot_ids


def selector(targets, shape, rows):
    matched = targets[None, :] == jnp.arange(rows, dtype=jnp.int32)[:, None]
    chosen = matched.reshape(rows, *shape)
    return jnp.sum(chosen.astype(jnp.float32), axis=2).astype(jnp.bfloat16)


def gate_up_parts(sets, weights):
    parts, _, width = weights.shape
    set_rows = sets[0].shape[0]
    rows = set_rows * len(sets)

    def kernel(*refs):
        set_refs, (w_ref, out_ref) = refs[: len(sets)], refs[len(sets) :]
        stacked = jnp.concatenate([ref[...] for ref in set_refs], axis=0)
        for part in range(parts):
            out_ref[part] = jnp.dot(stacked, w_ref[part], preferred_element_type=jnp.float32).astype(out_ref.dtype)

    return pl.pallas_call(
        kernel,
        out_shape=jax.ShapeDtypeStruct((parts, rows, width), jnp.bfloat16),
        in_specs=[VMEM] * (len(sets) + 1),
        out_specs=VMEM,
        compiler_params=LIMIT,
        name="gate_up_parts",
    )(*sets, weights)


def hidden_copies(parts):
    count, rows, both = parts.shape
    width = both // 2

    def kernel(in_ref, out_ref):
        total = in_ref[0].astype(jnp.float32)
        for part in range(1, count):
            total += in_ref[part].astype(jnp.float32)
        gate, up = total[:, :width], total[:, width:]
        hidden = (gate / (1.0 + jnp.exp(-gate)) * up).astype(out_ref.dtype)
        for part in range(count):
            out_ref[part] = hidden

    return pl.pallas_call(
        kernel,
        out_shape=jax.ShapeDtypeStruct((count, rows, width), jnp.bfloat16),
        in_specs=[VMEM],
        out_specs=VMEM,
        compiler_params=LIMIT,
        name="hidden_copies",
    )(parts)


def down_sets(hidden, w_down, count):
    parts, rows, _ = hidden.shape
    set_rows = rows // count
    features = w_down.shape[1]

    def kernel(hidden_ref, w_ref, *out_refs):
        wide = jnp.concatenate([hidden_ref[part] for part in range(parts)], axis=1)
        out = jnp.dot(wide, w_ref[...], preferred_element_type=jnp.float32)
        for place, ref in enumerate(out_refs):
            ref[...] = out[place * set_rows : (place + 1) * set_rows].astype(ref.dtype)

    return pl.pallas_call(
        kernel,
        out_shape=[
            jax.ShapeDtypeStruct((set_rows, features), jnp.bfloat16 if place else jnp.float32)
            for place in range(count)
        ],
        in_specs=[VMEM, VMEM],
        out_specs=[VMEM] * count,
        compiler_params=LIMIT,
        name="down_sets",
    )(hidden, w_down)


def per_device(
    tokens, expert_ids, route_weight, gate_weight, up_weight, down_weight, past_layers, dwa_weight
):
    experts = lax.axis_size("expert")
    parts = lax.axis_size("tensor")
    tok_rows, feature_width = tokens.shape
    chosen_count = expert_ids.shape[1]
    capacity = min(tok_rows, 3 * chosen_count * tok_rows // (2 * experts))
    quarter = feature_width // parts
    groups = far_groups(lax.axis_size("dp"))
    block = experts * capacity

    slabs = [w.reshape(parts, quarter, -1) for w in (gate_weight, up_weight)]
    w_both = lax.all_to_all(jnp.concatenate(slabs, axis=2), "tensor", 0, 0, tiled=True)

    targets = assignment_slots(expert_ids, experts, capacity)
    selected = selector(targets, expert_ids.shape, block)
    first_column = lax.axis_index("tensor") * quarter
    own_columns = lax.dynamic_slice_in_dim(tokens, first_column, quarter, 1)
    packed = jnp.dot(selected, own_columns, preferred_element_type=jnp.float32).astype(jnp.bfloat16)
    arrived = lax.all_to_all(packed.reshape(experts, capacity, quarter), "expert", 0, 0, tiled=True)
    far = lax.all_to_all(
        jnp.broadcast_to(arrived.reshape(1, block, quarter), (RADIX, block, quarter)),
        "dp",
        0,
        0,
        tiled=True,
        axis_index_groups=groups,
    ).reshape(RADIX * block, quarter)
    sets = [far, *from_neighbours(far)]

    partial = gate_up_parts(sets, w_both)
    partial = lax.all_to_all(partial, "tensor", 0, 0, tiled=True)
    hidden = lax.all_to_all(hidden_copies(partial), "tensor", 0, 0, tiled=True)
    own, *others = down_sets(hidden, down_weight[0], len(sets))
    for other in to_neighbours(others):
        own = own + other.astype(jnp.float32)
    own = own.astype(jnp.bfloat16).reshape(RADIX, block, quarter)
    own = lax.all_to_all(own, "dp", 0, 0, tiled=True, axis_index_groups=groups)
    expert_out = jnp.sum(own.astype(jnp.float32), axis=0).astype(jnp.bfloat16)
    returned_rows = lax.all_to_all(
        expert_out.reshape(experts, capacity, quarter), "expert", 0, 0, tiled=True
    ).reshape(block, quarter)

    fetched = returned_rows[targets].astype(jnp.float32).reshape(tok_rows, chosen_count, quarter)
    shares = route_weight / jnp.sum(route_weight, axis=1, keepdims=True)
    expert_mix = jnp.sum(fetched * shares[:, :, None], axis=1)
    current = own_columns.astype(jnp.float32) + expert_mix
    depth = past_layers.shape[0]
    history = jnp.einsum("j,jtd->td", dwa_weight[:depth], past_layers.astype(jnp.float32))
    return (dwa_weight[depth] * current + history).astype(jnp.bfloat16)


def solution(mesh):
    return jax.shard_map(
        per_device,
        mesh=mesh,
        in_specs=(
            P(("expert", "dp"), None),
            P(("expert", "dp"), None),
            P(("expert", "dp"), None),
            P("expert", None, ("dp", "tensor")),
            P("expert", None, ("dp", "tensor")),
            P("expert", "dp", "tensor"),
            P(None, ("expert", "dp"), "tensor"),
            P(),
        ),
        out_specs=P(("expert", "dp"), "tensor"),
        check_vma=False,
    )
```

```python
import jax
import jax.numpy as jnp
import numpy as np
from jax import lax
from jax.experimental import pallas as pl
from jax.experimental.pallas import tpu as pltpu
from jax.sharding import PartitionSpec as P

RADIX = 4
LANES = 128
SHIFTS = (0, 1, 3, 2)


LIMIT = pltpu.CompilerParams(vmem_limit_bytes=16 * 2**20)
SMEM = pl.BlockSpec(memory_space=pltpu.SMEM)
VMEM = pl.BlockSpec(memory_space=pltpu.VMEM)


def far_groups(count):
    stride = count // RADIX
    return [[low + stride * high for high in range(RADIX)] for low in range(stride)]


def shifted(shard, even_shift, odd_shift):
    experts, count = lax.axis_size("expert"), lax.axis_size("dp")
    pairs = []
    for expert in range(experts):
        shift = odd_shift if expert % 2 else even_shift
        for place in range(count):
            pairs.append((expert * count + place, expert * count + (place + shift) % count))
    return lax.ppermute(shard, ("expert", "dp"), pairs)


def to_neighbours(shards):
    above, second, below = shards
    return [shifted(above, 1, 1), shifted(below, -1, -1), shifted(second, 2, -2)]


def assignment_slots(expert_ids, experts, capacity):
    flat_ids = expert_ids.reshape(-1)
    matches = (flat_ids[:, None] == jnp.arange(experts, dtype=jnp.int32)[None, :]).astype(jnp.int32)
    earlier = jnp.cumsum(matches, axis=0) - matches
    slot_ids = jnp.sum(earlier * matches, axis=1)
    return flat_ids * capacity + slot_ids


def packed_rows(gathered, offset, feature_width, experts, capacity, chosen_count, block):
    rows = gathered.shape[0]
    groups = rows // block // RADIX
    set_rows = groups * capacity
    per_expert = RADIX * set_rows

    def kernel(offset_ref, in_ref, out_ref):
        labels = in_ref[:, feature_width:].astype(jnp.float32)
        lanes = labels.shape[1]
        lane = lax.broadcasted_iota(jnp.int32, (rows, lanes), 1).astype(jnp.float32)
        named = jnp.zeros((rows, lanes), jnp.float32)
        for place in range(chosen_count):
            named += (labels[:, place : place + 1] == lane).astype(jnp.float32)
        row = lax.broadcasted_iota(jnp.int32, (rows, rows), 0)
        column = lax.broadcasted_iota(jnp.int32, (rows, rows), 1)
        before = ((row // block == column // block) & (column < row)).astype(jnp.float32)
        earlier = jnp.dot(
            before.astype(jnp.bfloat16), named.astype(jnp.bfloat16), preferred_element_type=jnp.float32
        )
        source = lax.broadcasted_iota(jnp.int32, (rows, lanes), 0) // block
        residue = (source % RADIX - offset_ref[0] + RADIX) % RADIX
        first = (residue * set_rows + source // RADIX * capacity).astype(jnp.float32)
        target = jnp.where(named > 0.0, first + earlier, -1.0).T
        wanted = lax.broadcasted_iota(jnp.int32, (per_expert, rows), 0).astype(jnp.float32)
        chosen = [(wanted == target[expert : expert + 1, :]).astype(jnp.float32) for expert in range(experts)]
        chosen = jnp.concatenate(chosen, axis=0).astype(jnp.bfloat16)
        out = jnp.dot(chosen, in_ref[:, :feature_width], preferred_element_type=jnp.float32)
        out_ref[...] = out.astype(out_ref.dtype).reshape(out_ref.shape)

    return pl.pallas_call(
        kernel,
        out_shape=jax.ShapeDtypeStruct((experts, per_expert, feature_width), gathered.dtype),
        in_specs=[SMEM, VMEM],
        out_specs=VMEM,
        compiler_params=LIMIT,
        name="packed_rows",
    )(offset, gathered)


def weights_by_features(gate_weight, up_weight, quarter):
    parts = lax.axis_size("tensor")
    here = lax.axis_index("tensor")
    slabs = [w.reshape(parts, quarter, -1) for w in (gate_weight, up_weight)]

    def slab(shift):
        place = (here + shift) % parts
        both = [lax.dynamic_index_in_dim(w, place, 0, keepdims=False) for w in slabs]
        both = jnp.concatenate(both, axis=1)
        if shift == 0:
            return both
        return lax.ppermute(both, "tensor", [(i, (i + shift) % parts) for i in range(parts)])

    return [slab(shift) for shift in SHIFTS]


def gate_up_parts(rows, weights, place):
    parts = len(weights)
    width = weights[0].shape[1]
    count = rows.shape[0] * rows.shape[1]

    def kernel(place_ref, in_ref, *refs):
        w_refs, out_ref = refs[:-1], refs[-1]
        stacked = in_ref[...].reshape(count, in_ref.shape[2])
        for shift, w_ref in zip(SHIFTS, w_refs):
            part = (place_ref[0] + (parts - shift)) % parts
            out = jnp.dot(stacked, w_ref[...], preferred_element_type=jnp.float32)
            out_ref[part] = out.astype(out_ref.dtype)

    return pl.pallas_call(
        kernel,
        out_shape=jax.ShapeDtypeStruct((parts, count, width), jnp.bfloat16),
        in_specs=[SMEM] + [VMEM] * (1 + parts),
        out_specs=VMEM,
        compiler_params=LIMIT,
        name="gate_up_parts",
    )(place, rows, *weights)


def hidden_copies(parts):
    count, rows, both = parts.shape
    width = both // 2

    def kernel(in_ref, out_ref):
        total = in_ref[0].astype(jnp.float32)
        for part in range(1, count):
            total += in_ref[part].astype(jnp.float32)
        gate, up = total[:, :width], total[:, width:]
        hidden = (gate / (1.0 + jnp.exp(-gate)) * up).astype(out_ref.dtype)
        for part in range(count):
            out_ref[part] = hidden

    return pl.pallas_call(
        kernel,
        out_shape=jax.ShapeDtypeStruct((count, rows, width), jnp.bfloat16),
        in_specs=[VMEM],
        out_specs=VMEM,
        compiler_params=LIMIT,
        name="hidden_copies",
    )(parts)


def down_sets(hidden, w_down, experts):
    parts, rows, _ = hidden.shape
    set_rows = rows // RADIX
    piece = set_rows // experts
    features = w_down.shape[1]

    def kernel(hidden_ref, w_ref, *out_refs):
        wide = jnp.concatenate([hidden_ref[part] for part in range(parts)], axis=1)
        out = jnp.dot(wide, w_ref[...], preferred_element_type=jnp.float32)
        for place, ref in enumerate(out_refs):
            starts = [(expert * RADIX + place) * piece for expert in range(experts)]
            ref[...] = jnp.concatenate([out[at : at + piece] for at in starts], axis=0).astype(ref.dtype)

    return pl.pallas_call(
        kernel,
        out_shape=[
            jax.ShapeDtypeStruct((set_rows, features), jnp.bfloat16 if place else jnp.float32)
            for place in range(RADIX)
        ],
        in_specs=[VMEM, VMEM],
        out_specs=[VMEM] * RADIX,
        compiler_params=LIMIT,
        name="down_sets",
    )(hidden, w_down)


def summed_by_block(own, others, experts, capacity):
    rows, features = own.shape
    order = np.arange(rows).reshape(experts, RADIX, capacity).transpose(1, 0, 2).reshape(-1)
    moved = jnp.asarray(np.eye(rows)[order], jnp.bfloat16)

    def kernel(moved_ref, own_ref, *refs):
        other_refs, out_ref = refs[:-1], refs[-1]
        total = own_ref[...]
        for ref in other_refs:
            total += ref[...].astype(jnp.float32)
        out = jnp.dot(moved_ref[...], total.astype(jnp.bfloat16), preferred_element_type=jnp.float32)
        out_ref[...] = out.astype(out_ref.dtype).reshape(out_ref.shape)

    return pl.pallas_call(
        kernel,
        out_shape=jax.ShapeDtypeStruct((RADIX, rows // RADIX, features), jnp.bfloat16),
        in_specs=[VMEM] * (2 + len(others)),
        out_specs=VMEM,
        compiler_params=LIMIT,
        name="summed_by_block",
    )(moved, own, *others)


def per_device(
    tokens, expert_ids, route_weight, gate_weight, up_weight, down_weight, past_layers, dwa_weight
):
    experts = lax.axis_size("expert")
    parts = lax.axis_size("tensor")
    tok_rows, feature_width = tokens.shape
    chosen_count = expert_ids.shape[1]
    capacity = min(tok_rows, 3 * chosen_count * tok_rows // (2 * experts))
    quarter = feature_width // parts
    groups = far_groups(lax.axis_size("dp"))
    block = experts * capacity

    weights = weights_by_features(gate_weight, up_weight, quarter)
    first_column = lax.axis_index("tensor") * quarter
    own_columns = lax.dynamic_slice_in_dim(tokens, first_column, quarter, 1)
    labels = jnp.pad(expert_ids.astype(tokens.dtype), ((0, 0), (0, LANES - chosen_count)))
    gathered = lax.all_gather(jnp.concatenate([own_columns, labels], axis=1), "dp", axis=0, tiled=True)
    offset = (lax.axis_index("dp") % RADIX).reshape(1)
    packed = packed_rows(gathered, offset, quarter, experts, capacity, chosen_count, tok_rows)
    rows = lax.all_to_all(packed, "expert", 0, 0, tiled=True)

    partial = gate_up_parts(rows, weights, lax.axis_index("tensor").reshape(1))
    partial = lax.all_to_all(partial, "tensor", 0, 0, tiled=True)
    hidden = lax.all_to_all(hidden_copies(partial), "tensor", 0, 0, tiled=True)
    own, *others = down_sets(hidden, down_weight[0], experts)
    own = summed_by_block(own, to_neighbours(others), experts, capacity)
    own = lax.all_to_all(own, "dp", 0, 0, tiled=True, axis_index_groups=groups)
    expert_out = jnp.sum(own.astype(jnp.float32), axis=0).astype(jnp.bfloat16)
    returned_rows = lax.all_to_all(
        expert_out.reshape(experts, capacity, quarter), "expert", 0, 0, tiled=True
    ).reshape(block, quarter)

    targets = assignment_slots(expert_ids, experts, capacity)
    fetched = returned_rows[targets].astype(jnp.float32).reshape(tok_rows, chosen_count, quarter)
    shares = route_weight / jnp.sum(route_weight, axis=1, keepdims=True)
    expert_mix = jnp.sum(fetched * shares[:, :, None], axis=1)
    current = own_columns.astype(jnp.float32) + expert_mix
    depth = past_layers.shape[0]
    history = jnp.einsum("j,jtd->td", dwa_weight[:depth], past_layers.astype(jnp.float32))
    return (dwa_weight[depth] * current + history).astype(jnp.bfloat16)


def solution(mesh):
    return jax.shard_map(
        per_device,
        mesh=mesh,
        in_specs=(
            P(("expert", "dp"), None),
            P(("expert", "dp"), None),
            P(("expert", "dp"), None),
            P("expert", None, ("dp", "tensor")),
            P("expert", None, ("dp", "tensor")),
            P("expert", "dp", "tensor"),
            P(None, ("expert", "dp"), "tensor"),
            P(),
        ),
        out_specs=P(("expert", "dp"), "tensor"),
        check_vma=False,
    )
```

```python
import jax
import jax.numpy as jnp
import numpy as np
from jax import lax
from jax.experimental import pallas as pl
from jax.experimental.pallas import tpu as pltpu
from jax.sharding import PartitionSpec as P

RADIX = 4
LANES = 128
LIMIT = pltpu.CompilerParams(vmem_limit_bytes=16 * 2**20)
SMEM = pl.BlockSpec(memory_space=pltpu.SMEM)
VMEM = pl.BlockSpec(memory_space=pltpu.VMEM)


def far_groups():
    experts, count = lax.axis_size("expert"), lax.axis_size("dp")
    stride = count // RADIX
    return [
        [expert * count + low + stride * high for expert in range(experts) for high in range(RADIX)]
        for low in range(stride)
    ]


def far_exchange(chunks):
    return lax.all_to_all(chunks, ("expert", "dp"), 0, 0, tiled=True, axis_index_groups=far_groups())


def shifted(shard, even_shift, odd_shift):
    experts, count = lax.axis_size("expert"), lax.axis_size("dp")
    pairs = []
    for expert in range(experts):
        shift = odd_shift if expert % 2 else even_shift
        for place in range(count):
            pairs.append((expert * count + place, expert * count + (place + shift) % count))
    return lax.ppermute(shard, ("expert", "dp"), pairs)


def from_neighbours(shard):
    return [shifted(shard, 1, 1), shifted(shard, -1, -1), shifted(shard, 2, -2)]


def to_neighbours(shards):
    below, above, second = shards
    return [shifted(below, -1, -1), shifted(above, 1, 1), shifted(second, -2, 2)]


def call(kernel, name, out_shape, *operands, in_specs=None):
    many = isinstance(out_shape, list)
    return pl.pallas_call(
        kernel,
        out_shape=out_shape,
        in_specs=in_specs or [VMEM] * len(operands),
        out_specs=[VMEM] * len(out_shape) if many else VMEM,
        compiler_params=LIMIT,
        name=name,
    )(*operands)


def assigned_slots(ids, experts, tok_rows):
    choices, lanes = ids.shape
    expert = lax.broadcasted_iota(jnp.int32, (experts, lanes), 0)
    chosen = [ids[place : place + 1, :] == expert for place in range(choices)]
    named = sum(mask.astype(jnp.float32) for mask in chosen)
    source = lax.broadcasted_iota(jnp.int32, (lanes, lanes), 0)
    token = lax.broadcasted_iota(jnp.int32, (lanes, lanes), 1) % tok_rows
    before = (source < token).astype(jnp.float32)
    earlier = jnp.dot(named, before, preferred_element_type=jnp.float32)
    return [jnp.where(mask, earlier, -1.0) for mask in chosen]


def placed(slots, values, capacity, tok_rows):
    experts, lanes = slots[0].shape
    blocks = lanes // tok_rows
    shape = (capacity * blocks, lanes)
    row = lax.broadcasted_iota(jnp.int32, shape, 0)
    column = lax.broadcasted_iota(jnp.int32, shape, 1)
    same_block = row % blocks == column // tok_rows
    slot = (row // blocks).astype(jnp.float32)
    pieces = []
    for expert in range(experts):
        piece = jnp.zeros(shape, jnp.float32)
        for found, value in zip(slots, values):
            piece += jnp.where(same_block & (found[expert : expert + 1, :] == slot), value, 0.0)
        pieces.append(piece)
    return jnp.concatenate(pieces, axis=0)


def packed_rows(ids, own_columns, experts, capacity):
    tok_rows, features = own_columns.shape
    blocks = features // LANES

    def kernel(ids_ref, in_ref, out_ref):
        slots = assigned_slots(ids_ref[...], experts, tok_rows)
        chosen = placed(slots, [1.0] * len(slots), capacity, tok_rows).astype(jnp.bfloat16)
        tall = [in_ref[:, block * LANES : (block + 1) * LANES] for block in range(blocks)]
        out = jnp.dot(chosen, jnp.concatenate(tall, axis=0), preferred_element_type=jnp.float32)
        out = out.astype(out_ref.dtype)
        height = capacity * blocks
        for expert in range(experts):
            for far in range(RADIX):
                out_ref[expert * RADIX + far] = out[expert * height : (expert + 1) * height]

    shape = jax.ShapeDtypeStruct((experts * RADIX, capacity * blocks, LANES), own_columns.dtype)
    return call(kernel, "packed_rows", shape, ids, own_columns)


def chunk_order(chunks, capacity, blocks):
    count = chunks * capacity * blocks
    order = np.arange(count).reshape(chunks, capacity, blocks).transpose(2, 0, 1).reshape(-1)
    return np.eye(count, dtype=np.float32)[order]


def wide_rows(chunks, order, capacity):
    count, height, _ = chunks.shape
    blocks = height // capacity
    together = order.shape[0] // height
    rows = together * capacity

    def kernel(order_ref, in_ref, out_ref):
        for group in range(count // together):
            tall = in_ref[group * together : (group + 1) * together].reshape(together * height, LANES)
            out = jnp.dot(order_ref[...], tall, preferred_element_type=jnp.float32).astype(out_ref.dtype)
            for block in range(blocks):
                piece = out[block * rows : (block + 1) * rows]
                out_ref[group * rows : (group + 1) * rows, block * LANES : (block + 1) * LANES] = piece

    shape = jax.ShapeDtypeStruct((count * capacity, blocks * LANES), chunks.dtype)
    return call(kernel, "wide_rows", shape, order, chunks)


def summed_chunks(own, others, order, capacity):
    total_rows, features = own.shape
    blocks = features // LANES
    height = capacity * blocks
    together = order.shape[0] // height
    rows = together * capacity

    def kernel(order_ref, own_ref, *refs):
        other_refs, out_ref = refs[:-1], refs[-1]
        total = own_ref[...]
        for ref in other_refs:
            total += ref[...].astype(jnp.float32)
        total = total.astype(out_ref.dtype)
        for group in range(total_rows // rows):
            part = total[group * rows : (group + 1) * rows]
            tall = [part[:, block * LANES : (block + 1) * LANES] for block in range(blocks)]
            out = jnp.dot(order_ref[...], jnp.concatenate(tall, axis=0), preferred_element_type=jnp.float32)
            out = out.astype(out_ref.dtype).reshape(together, height, LANES)
            out_ref[group * together : (group + 1) * together] = out

    shape = jax.ShapeDtypeStruct((total_rows // capacity, height, LANES), jnp.bfloat16)
    return call(kernel, "summed_chunks", shape, order, own, *others)


def gate_up_parts(sets, weights):
    parts, _, width = weights.shape
    set_rows = sets[0].shape[0]
    rows = set_rows * len(sets)

    def kernel(*refs):
        set_refs, (w_ref, out_ref) = refs[: len(sets)], refs[len(sets) :]
        stacked = jnp.concatenate([ref[...] for ref in set_refs], axis=0)
        for part in range(parts):
            out = jnp.dot(stacked, w_ref[part], preferred_element_type=jnp.float32)
            out_ref[part] = out.astype(out_ref.dtype)

    shape = jax.ShapeDtypeStruct((parts, rows, width), jnp.bfloat16)
    return call(kernel, "gate_up_parts", shape, *sets, weights)


def hidden_copies(parts):
    count, rows, both = parts.shape
    width = both // 2

    def kernel(in_ref, out_ref):
        total = in_ref[0].astype(jnp.float32)
        for part in range(1, count):
            total += in_ref[part].astype(jnp.float32)
        gate, up = total[:, :width], total[:, width:]
        hidden = (gate / (1.0 + jnp.exp(-gate)) * up).astype(out_ref.dtype)
        for part in range(count):
            out_ref[part] = hidden

    return call(kernel, "hidden_copies", jax.ShapeDtypeStruct((count, rows, width), jnp.bfloat16), parts)


def down_sets(hidden, w_down, count):
    parts, rows, _ = hidden.shape
    set_rows = rows // count
    features = w_down.shape[1]

    def kernel(hidden_ref, w_ref, *out_refs):
        wide = jnp.concatenate([hidden_ref[part] for part in range(parts)], axis=1)
        out = jnp.dot(wide, w_ref[...], preferred_element_type=jnp.float32)
        for place, ref in enumerate(out_refs):
            ref[...] = out[place * set_rows : (place + 1) * set_rows].astype(ref.dtype)

    shapes = [
        jax.ShapeDtypeStruct((set_rows, features), jnp.bfloat16 if place else jnp.float32)
        for place in range(count)
    ]
    return call(kernel, "down_sets", shapes, hidden, w_down)


def mixed_layers(returned, ids, route, own_columns, past_layers, dwa_weight, experts, capacity):
    tok_rows, features = own_columns.shape
    blocks = features // LANES
    height = capacity * blocks
    depth = past_layers.shape[0]

    def kernel(dwa_ref, ids_ref, route_ref, own_ref, past_ref, in_ref, out_ref):
        outs = []
        for expert in range(experts):
            total = in_ref[expert * RADIX].astype(jnp.float32)
            for far in range(1, RADIX):
                total += in_ref[expert * RADIX + far].astype(jnp.float32)
            outs.append(total.astype(jnp.bfloat16))
        outs = jnp.concatenate(outs, axis=0)
        slots = assigned_slots(ids_ref[...], experts, tok_rows)
        route = route_ref[...]
        total = sum(route[place : place + 1, :] for place in range(len(slots)))
        shares = [route[place : place + 1, :] / total for place in range(len(slots))]
        rest = placed(slots, shares, capacity, tok_rows)
        mix = jnp.zeros((blocks * tok_rows, LANES), jnp.float32)
        for _ in range(3):
            term = rest.astype(jnp.bfloat16)
            rest = rest - term.astype(jnp.float32)
            mix += lax.dot_general(term, outs, (((0,), (0,)), ((), ())), preferred_element_type=jnp.float32)
        for block in range(blocks):
            lanes = slice(block * LANES, (block + 1) * LANES)
            current = own_ref[:, lanes].astype(jnp.float32) + mix[block * tok_rows : (block + 1) * tok_rows]
            value = dwa_ref[depth] * current
            for layer in range(depth):
                value += dwa_ref[layer] * past_ref[layer, :, lanes].astype(jnp.float32)
            out_ref[:, lanes] = value.astype(out_ref.dtype)

    return call(
        kernel,
        "mixed_layers",
        jax.ShapeDtypeStruct((tok_rows, features), own_columns.dtype),
        dwa_weight,
        ids,
        route,
        own_columns,
        past_layers,
        returned,
        in_specs=[SMEM] + [VMEM] * 5,
    )


def per_device(
    tokens, expert_ids, route_weight, gate_weight, up_weight, down_weight, past_layers, dwa_weight
):
    experts = lax.axis_size("expert")
    parts = lax.axis_size("tensor")
    tok_rows, feature_width = tokens.shape
    chosen_count = expert_ids.shape[1]
    capacity = min(tok_rows, 3 * chosen_count * tok_rows // (2 * experts))
    quarter = feature_width // parts
    blocks = quarter // LANES
    together = 2 * RADIX
    order = chunk_order(together, capacity, blocks)
    ids = jnp.tile(expert_ids.T, (1, blocks))
    route = jnp.tile(route_weight.T, (1, blocks))
    first_column = lax.axis_index("tensor") * quarter
    own_columns = lax.dynamic_slice_in_dim(tokens, first_column, quarter, 1)

    slabs = [w.reshape(parts, quarter, -1) for w in (gate_weight, up_weight)]
    weights = lax.all_to_all(jnp.concatenate(slabs, axis=2), "tensor", 0, 0, tiled=True)

    arrived = far_exchange(packed_rows(ids, own_columns, experts, capacity))
    own_set = wide_rows(arrived, jnp.asarray(order, jnp.bfloat16), capacity)
    sets = [own_set, *from_neighbours(own_set)]
    partial = lax.all_to_all(gate_up_parts(sets, weights), "tensor", 0, 0, tiled=True)
    hidden = lax.all_to_all(hidden_copies(partial), "tensor", 0, 0, tiled=True)
    own, *others = down_sets(hidden, down_weight[0], len(sets))
    summed = summed_chunks(own, to_neighbours(others), jnp.asarray(order.T, jnp.bfloat16), capacity)
    returned = far_exchange(summed)
    return mixed_layers(
        returned, ids, route, own_columns, past_layers, dwa_weight, experts, capacity
    )


def solution(mesh):
    return jax.shard_map(
        per_device,
        mesh=mesh,
        in_specs=(
            P(("expert", "dp"), None),
            P(("expert", "dp"), None),
            P(("expert", "dp"), None),
            P("expert", None, ("dp", "tensor")),
            P("expert", None, ("dp", "tensor")),
            P("expert", "dp", "tensor"),
            P(None, ("expert", "dp"), "tensor"),
            P(),
        ),
        out_specs=P(("expert", "dp"), "tensor"),
        check_vma=False,
    )
```

```python
import jax
import jax.numpy as jnp
import numpy as np
from jax import lax
from jax.experimental import pallas as pl
from jax.experimental.pallas import tpu as pltpu
from jax.sharding import PartitionSpec as P

RADIX = 4
LANES = 128
SHIFTS = (0, 1, 3, 2)
LIMIT = pltpu.CompilerParams(vmem_limit_bytes=16 * 2**20)
SMEM = pl.BlockSpec(memory_space=pltpu.SMEM)
VMEM = pl.BlockSpec(memory_space=pltpu.VMEM)


def far_groups():
    experts, count = lax.axis_size("expert"), lax.axis_size("dp")
    stride = count // RADIX
    return [
        [expert * count + low + stride * high for expert in range(experts) for high in range(RADIX)]
        for low in range(stride)
    ]


def far_exchange(chunks):
    return lax.all_to_all(chunks, ("expert", "dp"), 0, 0, tiled=True, axis_index_groups=far_groups())


def shifted(shard, even_shift, odd_shift):
    experts, count = lax.axis_size("expert"), lax.axis_size("dp")
    pairs = []
    for expert in range(experts):
        shift = odd_shift if expert % 2 else even_shift
        for place in range(count):
            pairs.append((expert * count + place, expert * count + (place + shift) % count))
    return lax.ppermute(shard, ("expert", "dp"), pairs)


def from_neighbours(shard):
    return [shifted(shard, 1, 1), shifted(shard, -1, -1), shifted(shard, 2, -2)]


def to_neighbours(shards):
    below, above, second = shards
    return [shifted(below, -1, -1), shifted(above, 1, 1), shifted(second, -2, 2)]


def call(kernel, name, out_shape, *operands, in_specs=None):
    many = isinstance(out_shape, list)
    return pl.pallas_call(
        kernel,
        out_shape=out_shape,
        in_specs=in_specs or [VMEM] * len(operands),
        out_specs=[VMEM] * len(out_shape) if many else VMEM,
        compiler_params=LIMIT,
        name=name,
    )(*operands)


def repeated_ids(ids):
    tok_rows = ids.shape[1]
    token = lax.broadcasted_iota(jnp.int32, (tok_rows, LANES), 0)
    lane = lax.broadcasted_iota(jnp.int32, (tok_rows, LANES), 1)
    spread = (lane % tok_rows == token).astype(jnp.float32)
    return jnp.dot(ids.astype(jnp.float32), spread, preferred_element_type=jnp.float32)


def assigned_slots(ids, experts, tok_rows):
    ids = repeated_ids(ids)
    choices, lanes = ids.shape
    expert = lax.broadcasted_iota(jnp.int32, (experts, lanes), 0).astype(jnp.float32)
    chosen = [ids[place : place + 1, :] == expert for place in range(choices)]
    named = sum(mask.astype(jnp.float32) for mask in chosen)
    source = lax.broadcasted_iota(jnp.int32, (lanes, lanes), 0)
    token = lax.broadcasted_iota(jnp.int32, (lanes, lanes), 1) % tok_rows
    before = (source < token).astype(jnp.float32)
    earlier = jnp.dot(named, before, preferred_element_type=jnp.float32)
    return [jnp.where(mask, earlier, -1.0) for mask in chosen]


def placed(slots, values, capacity, tok_rows):
    experts, lanes = slots[0].shape
    blocks = lanes // tok_rows
    shape = (capacity * blocks, lanes)
    row = lax.broadcasted_iota(jnp.int32, shape, 0)
    column = lax.broadcasted_iota(jnp.int32, shape, 1)
    same_block = row % blocks == column // tok_rows
    slot = (row // blocks).astype(jnp.float32)
    pieces = []
    for expert in range(experts):
        piece = jnp.zeros(shape, jnp.float32)
        for found, value in zip(slots, values):
            piece += jnp.where(same_block & (found[expert : expert + 1, :] == slot), value, 0.0)
        pieces.append(piece)
    return jnp.concatenate(pieces, axis=0)


def packed_rows(ids, own_columns, experts, capacity):
    tok_rows, features = own_columns.shape
    blocks = features // LANES

    def kernel(ids_ref, in_ref, out_ref):
        slots = assigned_slots(ids_ref[...], experts, tok_rows)
        chosen = placed(slots, [1.0] * len(slots), capacity, tok_rows).astype(jnp.bfloat16)
        tall = [in_ref[:, block * LANES : (block + 1) * LANES] for block in range(blocks)]
        out = jnp.dot(chosen, jnp.concatenate(tall, axis=0), preferred_element_type=jnp.float32)
        out = out.astype(out_ref.dtype)
        height = capacity * blocks
        for expert in range(experts):
            for far in range(RADIX):
                out_ref[expert * RADIX + far] = out[expert * height : (expert + 1) * height]

    shape = jax.ShapeDtypeStruct((experts * RADIX, capacity * blocks, LANES), own_columns.dtype)
    return call(kernel, "packed_rows", shape, ids, own_columns)


def chunk_order(chunks, capacity, blocks):
    count = chunks * capacity * blocks
    order = np.arange(count).reshape(chunks, capacity, blocks).transpose(2, 0, 1).reshape(-1)
    return np.eye(count, dtype=np.float32)[order]


def wide_rows(chunks, order, capacity):
    count, height, _ = chunks.shape
    blocks = height // capacity
    together = order.shape[0] // height
    rows = together * capacity

    def kernel(order_ref, in_ref, out_ref):
        for group in range(count // together):
            tall = in_ref[group * together : (group + 1) * together].reshape(together * height, LANES)
            out = jnp.dot(order_ref[...], tall, preferred_element_type=jnp.float32).astype(out_ref.dtype)
            for block in range(blocks):
                piece = out[block * rows : (block + 1) * rows]
                out_ref[group * rows : (group + 1) * rows, block * LANES : (block + 1) * LANES] = piece

    shape = jax.ShapeDtypeStruct((count * capacity, blocks * LANES), chunks.dtype)
    return call(kernel, "wide_rows", shape, order, chunks)


def summed_chunks(own, others, order, capacity):
    total_rows, features = own.shape
    blocks = features // LANES
    height = capacity * blocks
    together = order.shape[0] // height
    rows = together * capacity

    def kernel(order_ref, own_ref, *refs):
        other_refs, out_ref = refs[:-1], refs[-1]
        total = own_ref[...]
        for ref in other_refs:
            total += ref[...].astype(jnp.float32)
        total = total.astype(out_ref.dtype)
        for group in range(total_rows // rows):
            part = total[group * rows : (group + 1) * rows]
            tall = [part[:, block * LANES : (block + 1) * LANES] for block in range(blocks)]
            out = jnp.dot(order_ref[...], jnp.concatenate(tall, axis=0), preferred_element_type=jnp.float32)
            out = out.astype(out_ref.dtype).reshape(together, height, LANES)
            out_ref[group * together : (group + 1) * together] = out

    shape = jax.ShapeDtypeStruct((total_rows // capacity, height, LANES), jnp.bfloat16)
    return call(kernel, "summed_chunks", shape, order, own, *others)


def weights_by_features(gate_weight, up_weight, quarter):
    parts = lax.axis_size("tensor")
    here = lax.axis_index("tensor")
    slabs = [w.reshape(parts, quarter, -1) for w in (gate_weight, up_weight)]

    def slab(shift):
        place = (here + shift) % parts
        both = [lax.dynamic_index_in_dim(w, place, 0, keepdims=False) for w in slabs]
        both = jnp.concatenate(both, axis=1)
        if shift == 0:
            return both
        return lax.ppermute(both, "tensor", [(i, (i + shift) % parts) for i in range(parts)])

    return [slab(shift) for shift in SHIFTS]


def gate_up_parts(sets, weights, place):
    parts = len(weights)
    width = weights[0].shape[1]
    set_rows = sets[0].shape[0]
    rows = set_rows * len(sets)

    def kernel(place_ref, *refs):
        set_refs, w_refs, out_ref = refs[: len(sets)], refs[len(sets) : -1], refs[-1]
        stacked = jnp.concatenate([ref[...] for ref in set_refs], axis=0)
        for shift, w_ref in zip(SHIFTS, w_refs):
            part = (place_ref[0] + (parts - shift)) % parts
            out = jnp.dot(stacked, w_ref[...], preferred_element_type=jnp.float32)
            out_ref[part] = out.astype(out_ref.dtype)

    shape = jax.ShapeDtypeStruct((parts, rows, width), jnp.bfloat16)
    specs = [SMEM] + [VMEM] * (len(sets) + parts)
    return call(kernel, "gate_up_parts", shape, place, *sets, *weights, in_specs=specs)


def hidden_units(parts):
    count, rows, both = parts.shape
    width = both // 2

    def kernel(in_ref, out_ref):
        total = in_ref[0].astype(jnp.float32)
        for part in range(1, count):
            total += in_ref[part].astype(jnp.float32)
        gate, up = total[:, :width], total[:, width:]
        out_ref[...] = (gate / (1.0 + jnp.exp(-gate)) * up).astype(out_ref.dtype)

    return call(kernel, "hidden_units", jax.ShapeDtypeStruct((rows, width), jnp.bfloat16), parts)


def down_sets(hidden, w_down, count):
    parts, rows, _ = hidden.shape
    set_rows = rows // count
    features = w_down.shape[1]

    def kernel(hidden_ref, w_ref, *out_refs):
        wide = jnp.concatenate([hidden_ref[part] for part in range(parts)], axis=1)
        out = jnp.dot(wide, w_ref[...], preferred_element_type=jnp.float32)
        for place, ref in enumerate(out_refs):
            ref[...] = out[place * set_rows : (place + 1) * set_rows].astype(ref.dtype)

    shapes = [
        jax.ShapeDtypeStruct((set_rows, features), jnp.bfloat16 if place else jnp.float32)
        for place in range(count)
    ]
    return call(kernel, "down_sets", shapes, hidden, w_down)


def mixed_layers(returned, ids, route, own_columns, past_layers, dwa_weight, experts, capacity):
    tok_rows, features = own_columns.shape
    blocks = features // LANES
    height = capacity * blocks
    depth = past_layers.shape[0]

    def kernel(dwa_ref, ids_ref, route_ref, own_ref, past_ref, in_ref, out_ref):
        outs = []
        for expert in range(experts):
            total = in_ref[expert * RADIX].astype(jnp.float32)
            for far in range(1, RADIX):
                total += in_ref[expert * RADIX + far].astype(jnp.float32)
            outs.append(total.astype(jnp.bfloat16))
        outs = jnp.concatenate(outs, axis=0)
        slots = assigned_slots(ids_ref[...], experts, tok_rows)
        route = route_ref[...]
        total = sum(route[place : place + 1, :] for place in range(len(slots)))
        shares = [route[place : place + 1, :] / total for place in range(len(slots))]
        rest = placed(slots, shares, capacity, tok_rows)
        mix = jnp.zeros((blocks * tok_rows, LANES), jnp.float32)
        for _ in range(3):
            term = rest.astype(jnp.bfloat16)
            rest = rest - term.astype(jnp.float32)
            mix += lax.dot_general(term, outs, (((0,), (0,)), ((), ())), preferred_element_type=jnp.float32)
        for block in range(blocks):
            lanes = slice(block * LANES, (block + 1) * LANES)
            current = own_ref[:, lanes].astype(jnp.float32) + mix[block * tok_rows : (block + 1) * tok_rows]
            value = dwa_ref[depth] * current
            for layer in range(depth):
                value += dwa_ref[layer] * past_ref[layer, :, lanes].astype(jnp.float32)
            out_ref[:, lanes] = value.astype(out_ref.dtype)

    return call(
        kernel,
        "mixed_layers",
        jax.ShapeDtypeStruct((tok_rows, features), own_columns.dtype),
        dwa_weight,
        ids,
        route,
        own_columns,
        past_layers,
        returned,
        in_specs=[SMEM] + [VMEM] * 5,
    )


def per_device(
    tokens, expert_ids, route_weight, gate_weight, up_weight, down_weight, past_layers, dwa_weight
):
    experts = lax.axis_size("expert")
    parts = lax.axis_size("tensor")
    tok_rows, feature_width = tokens.shape
    chosen_count = expert_ids.shape[1]
    capacity = min(tok_rows, 3 * chosen_count * tok_rows // (2 * experts))
    quarter = feature_width // parts
    blocks = quarter // LANES
    together = 2 * RADIX
    order = chunk_order(together, capacity, blocks)
    ids = expert_ids.T
    route = jnp.tile(route_weight.T, (1, blocks))
    first_column = lax.axis_index("tensor") * quarter
    own_columns = lax.dynamic_slice_in_dim(tokens, first_column, quarter, 1)

    weights = weights_by_features(gate_weight, up_weight, quarter)
    place = lax.axis_index("tensor").reshape(1)
    arrived = far_exchange(packed_rows(ids, own_columns, experts, capacity))
    own_set = wide_rows(arrived, jnp.asarray(order, jnp.bfloat16), capacity)
    sets = [own_set, *from_neighbours(own_set)]
    partial = lax.all_to_all(gate_up_parts(sets, weights, place), "tensor", 0, 0, tiled=True)
    hidden = lax.all_gather(hidden_units(partial), "tensor", axis=0, tiled=False)
    own, *others = down_sets(hidden, down_weight[0], len(sets))
    summed = summed_chunks(own, to_neighbours(others), jnp.asarray(order.T, jnp.bfloat16), capacity)
    returned = far_exchange(summed)
    return mixed_layers(
        returned, ids, route, own_columns, past_layers, dwa_weight, experts, capacity
    )


def solution(mesh):
    return jax.shard_map(
        per_device,
        mesh=mesh,
        in_specs=(
            P(("expert", "dp"), None),
            P(("expert", "dp"), None),
            P(("expert", "dp"), None),
            P("expert", None, ("dp", "tensor")),
            P("expert", None, ("dp", "tensor")),
            P("expert", "dp", "tensor"),
            P(None, ("expert", "dp"), "tensor"),
            P(),
        ),
        out_specs=P(("expert", "dp"), "tensor"),
        check_vma=False,
    )
```

```python
import jax
import jax.numpy as jnp
import numpy as np
from jax import lax
from jax.experimental import pallas as pl
from jax.experimental.pallas import tpu as pltpu
from jax.sharding import PartitionSpec as P

RADIX = 4
LANES = 128
SHIFTS = (0, 1, 3, 2)
LIMIT = pltpu.CompilerParams(vmem_limit_bytes=16 * 2**20)
SMEM = pl.BlockSpec(memory_space=pltpu.SMEM)
VMEM = pl.BlockSpec(memory_space=pltpu.VMEM)


def far_groups():
    experts, count = lax.axis_size("expert"), lax.axis_size("dp")
    stride = count // RADIX
    return [
        [expert * count + low + stride * high for expert in range(experts) for high in range(RADIX)]
        for low in range(stride)
    ]


def far_exchange(chunks):
    return lax.all_to_all(chunks, ("expert", "dp"), 0, 0, tiled=True, axis_index_groups=far_groups())


def shifted(shard, even_shift, odd_shift):
    experts, count = lax.axis_size("expert"), lax.axis_size("dp")
    pairs = []
    for expert in range(experts):
        shift = odd_shift if expert % 2 else even_shift
        for place in range(count):
            pairs.append((expert * count + place, expert * count + (place + shift) % count))
    return lax.ppermute(shard, ("expert", "dp"), pairs)


def from_neighbours(shard):
    return [shifted(shard, 1, 1), shifted(shard, -1, -1), shifted(shard, 2, -2)]


def to_neighbours(below, above, second):
    return [shifted(below, -1, -1), shifted(above, 1, 1), shifted(second, -2, 2)]


def call(kernel, out_shape, *operands, in_specs=None):
    many = isinstance(out_shape, list)
    return pl.pallas_call(
        kernel,
        out_shape=out_shape,
        in_specs=in_specs or [VMEM] * len(operands),
        out_specs=[VMEM] * len(out_shape) if many else VMEM,
        compiler_params=LIMIT,
    )(*operands)


def repeated_ids(ids):
    tok_rows = ids.shape[1]
    token = lax.broadcasted_iota(jnp.int32, (tok_rows, LANES), 0)
    lane = lax.broadcasted_iota(jnp.int32, (tok_rows, LANES), 1)
    spread = (lane % tok_rows == token).astype(jnp.float32)
    return jnp.dot(ids.astype(jnp.float32), spread, preferred_element_type=jnp.float32)


def assigned_slots(ids, experts, tok_rows):
    ids = repeated_ids(ids)
    choices, lanes = ids.shape
    expert = lax.broadcasted_iota(jnp.int32, (experts, lanes), 0).astype(jnp.float32)
    chosen = [ids[place : place + 1, :] == expert for place in range(choices)]
    named = sum(mask.astype(jnp.float32) for mask in chosen)
    source = lax.broadcasted_iota(jnp.int32, (lanes, lanes), 0)
    token = lax.broadcasted_iota(jnp.int32, (lanes, lanes), 1) % tok_rows
    before = (source < token).astype(jnp.float32)
    earlier = jnp.dot(named, before, preferred_element_type=jnp.float32)
    return [jnp.where(mask, earlier, -1.0) for mask in chosen]


def placed(slots, values, capacity, tok_rows):
    experts, lanes = slots[0].shape
    blocks = lanes // tok_rows
    shape = (capacity * blocks, lanes)
    row = lax.broadcasted_iota(jnp.int32, shape, 0)
    column = lax.broadcasted_iota(jnp.int32, shape, 1)
    same_block = row % blocks == column // tok_rows
    slot = (row // blocks).astype(jnp.float32)
    pieces = []
    for expert in range(experts):
        piece = jnp.zeros(shape, jnp.float32)
        for found, value in zip(slots, values):
            piece += jnp.where(same_block & (found[expert : expert + 1, :] == slot), value, 0.0)
        pieces.append(piece)
    return jnp.concatenate(pieces, axis=0)


def packed_rows(ids, own_columns, experts, capacity):
    tok_rows, features = own_columns.shape
    blocks = features // LANES

    def kernel(ids_ref, in_ref, out_ref):
        slots = assigned_slots(ids_ref[...], experts, tok_rows)
        chosen = placed(slots, [1.0] * len(slots), capacity, tok_rows).astype(jnp.bfloat16)
        tall = [in_ref[:, block * LANES : (block + 1) * LANES] for block in range(blocks)]
        out = jnp.dot(chosen, jnp.concatenate(tall, axis=0), preferred_element_type=jnp.float32)
        out = out.astype(out_ref.dtype)
        height = capacity * blocks
        for expert in range(experts):
            for far in range(RADIX):
                out_ref[expert * RADIX + far] = out[expert * height : (expert + 1) * height]

    shape = jax.ShapeDtypeStruct((experts * RADIX, capacity * blocks, LANES), own_columns.dtype)
    return call(kernel, shape, ids, own_columns)


def chunk_order(chunks, capacity, blocks):
    count = chunks * capacity * blocks
    order = np.arange(count).reshape(chunks, capacity, blocks).transpose(2, 0, 1).reshape(-1)
    return np.eye(count, dtype=np.float32)[order]


def wide_rows(chunks, order, capacity):
    count, height, _ = chunks.shape
    blocks = height // capacity
    together = order.shape[0] // height
    rows = together * capacity

    def kernel(order_ref, in_ref, out_ref):
        for group in range(count // together):
            tall = in_ref[group * together : (group + 1) * together].reshape(together * height, LANES)
            out = jnp.dot(order_ref[...], tall, preferred_element_type=jnp.float32).astype(out_ref.dtype)
            for block in range(blocks):
                piece = out[block * rows : (block + 1) * rows]
                out_ref[group * rows : (group + 1) * rows, block * LANES : (block + 1) * LANES] = piece

    shape = jax.ShapeDtypeStruct((count * capacity, blocks * LANES), chunks.dtype)
    return call(kernel, shape, order, chunks)


def summed_chunks(own, others, order, capacity):
    total_rows, features = own.shape
    blocks = features // LANES
    height = capacity * blocks
    together = order.shape[0] // height
    rows = together * capacity

    def kernel(order_ref, own_ref, *refs):
        other_refs, out_ref = refs[:-1], refs[-1]
        total = own_ref[...]
        for ref in other_refs:
            total += ref[...].astype(jnp.float32)
        total = total.astype(out_ref.dtype)
        for group in range(total_rows // rows):
            part = total[group * rows : (group + 1) * rows]
            tall = [part[:, block * LANES : (block + 1) * LANES] for block in range(blocks)]
            out = jnp.dot(order_ref[...], jnp.concatenate(tall, axis=0), preferred_element_type=jnp.float32)
            out = out.astype(out_ref.dtype).reshape(together, height, LANES)
            out_ref[group * together : (group + 1) * together] = out

    shape = jax.ShapeDtypeStruct((total_rows // capacity, height, LANES), jnp.bfloat16)
    return call(kernel, shape, order, own, *others)


def weights_by_features(gate_weight, up_weight, quarter):
    parts = lax.axis_size("tensor")
    here = lax.axis_index("tensor")
    slabs = [w.reshape(parts, quarter, -1) for w in (gate_weight, up_weight)]

    def slab(shift):
        place = (here + shift) % parts
        both = [lax.dynamic_index_in_dim(w, place, 0, keepdims=False) for w in slabs]
        both = jnp.concatenate(both, axis=1)
        if shift == 0:
            return both
        return lax.ppermute(both, "tensor", [(i, (i + shift) % parts) for i in range(parts)])

    return [slab(shift) for shift in SHIFTS]


def gate_up_parts(sets, weights, place):
    parts = len(weights)
    width = weights[0].shape[1]
    set_rows = sets[0].shape[0]
    rows = set_rows * len(sets)

    def kernel(place_ref, *refs):
        set_refs, w_refs, out_ref = refs[: len(sets)], refs[len(sets) : -1], refs[-1]
        stacked = jnp.concatenate([ref[...] for ref in set_refs], axis=0)
        for shift, w_ref in zip(SHIFTS, w_refs):
            part = (place_ref[0] + (parts - shift)) % parts
            out = jnp.dot(stacked, w_ref[...], preferred_element_type=jnp.float32)
            out_ref[part] = out.astype(out_ref.dtype)

    shape = jax.ShapeDtypeStruct((parts, rows, width), jnp.bfloat16)
    specs = [SMEM] + [VMEM] * (len(sets) + parts)
    return call(kernel, shape, place, *sets, *weights, in_specs=specs)


def hidden_units(parts):
    count, rows, both = parts.shape
    width = both // 2

    def kernel(in_ref, out_ref):
        total = in_ref[0].astype(jnp.float32)
        for part in range(1, count):
            total += in_ref[part].astype(jnp.float32)
        gate, up = total[:, :width], total[:, width:]
        out_ref[...] = (gate / (1.0 + jnp.exp(-gate)) * up).astype(out_ref.dtype)

    return call(kernel, jax.ShapeDtypeStruct((rows, width), jnp.bfloat16), parts)


def down_sets(hidden, w_down, dtypes):
    parts, rows, _ = hidden.shape
    set_rows = rows // len(dtypes)
    features = w_down.shape[1]

    def kernel(hidden_ref, w_ref, *out_refs):
        wide = jnp.concatenate([hidden_ref[part] for part in range(parts)], axis=1)
        out = jnp.dot(wide, w_ref[...], preferred_element_type=jnp.float32)
        for place, ref in enumerate(out_refs):
            ref[...] = out[place * set_rows : (place + 1) * set_rows].astype(ref.dtype)

    shapes = [jax.ShapeDtypeStruct((set_rows, features), dtype) for dtype in dtypes]
    return call(kernel, shapes, hidden, w_down)


def mixed_layers(returned, ids, route, own_columns, past_layers, dwa_weight, experts, capacity):
    tok_rows, features = own_columns.shape
    blocks = features // LANES
    depth = past_layers.shape[0]

    def kernel(dwa_ref, ids_ref, route_ref, own_ref, past_ref, in_ref, out_ref):
        outs = []
        for expert in range(experts):
            total = in_ref[expert * RADIX].astype(jnp.float32)
            for far in range(1, RADIX):
                total += in_ref[expert * RADIX + far].astype(jnp.float32)
            outs.append(total.astype(jnp.bfloat16))
        outs = jnp.concatenate(outs, axis=0)
        slots = assigned_slots(ids_ref[...], experts, tok_rows)
        route = route_ref[...]
        total = sum(route[place : place + 1, :] for place in range(len(slots)))
        shares = [route[place : place + 1, :] / total for place in range(len(slots))]
        rest = placed(slots, shares, capacity, tok_rows)
        mix = jnp.zeros((blocks * tok_rows, LANES), jnp.float32)
        for _ in range(3):
            term = rest.astype(jnp.bfloat16)
            rest = rest - term.astype(jnp.float32)
            mix += lax.dot_general(term, outs, (((0,), (0,)), ((), ())), preferred_element_type=jnp.float32)
        for block in range(blocks):
            lanes = slice(block * LANES, (block + 1) * LANES)
            current = own_ref[:, lanes].astype(jnp.float32) + mix[block * tok_rows : (block + 1) * tok_rows]
            value = dwa_ref[depth] * current
            for layer in range(depth):
                value += dwa_ref[layer] * past_ref[layer, :, lanes].astype(jnp.float32)
            out_ref[:, lanes] = value.astype(out_ref.dtype)

    return call(
        kernel,
        jax.ShapeDtypeStruct((tok_rows, features), own_columns.dtype),
        dwa_weight,
        ids,
        route,
        own_columns,
        past_layers,
        returned,
        in_specs=[SMEM] + [VMEM] * 5,
    )


def per_device(
    tokens, expert_ids, route_weight, gate_weight, up_weight, down_weight, past_layers, dwa_weight
):
    experts = lax.axis_size("expert")
    parts = lax.axis_size("tensor")
    tok_rows, feature_width = tokens.shape
    chosen_count = expert_ids.shape[1]
    capacity = min(tok_rows, 3 * chosen_count * tok_rows // (2 * experts))
    quarter = feature_width // parts
    blocks = quarter // LANES
    together = 2 * RADIX
    order = chunk_order(together, capacity, blocks)
    ids = expert_ids.T
    route = jnp.tile(route_weight.T, (1, blocks))
    first_column = lax.axis_index("tensor") * quarter
    own_columns = lax.dynamic_slice_in_dim(tokens, first_column, quarter, 1)

    weights = weights_by_features(gate_weight, up_weight, quarter)
    place = lax.axis_index("tensor").reshape(1)
    arrived = far_exchange(packed_rows(ids, own_columns, experts, capacity))
    own_set = wide_rows(arrived, jnp.asarray(order, jnp.bfloat16), capacity)
    below, above, second = from_neighbours(own_set)

    def hidden_part(sets):
        partial = gate_up_parts(sets, weights, place)
        return hidden_units(lax.all_to_all(partial, "tensor", 0, 0, tiled=True))

    def outputs(hidden, dtypes):
        wide = lax.all_gather(hidden, "tensor", axis=0, tiled=False)
        return down_sets(wide, down_weight[0], dtypes)

    near_hidden = hidden_part([own_set, below])
    late_hidden = hidden_part([above, second])
    above, second = outputs(late_hidden, [jnp.bfloat16] * 2)
    near_hidden, above, second = lax.optimization_barrier((near_hidden, above, second))
    own, below = outputs(near_hidden, [jnp.float32, jnp.bfloat16])
    others = to_neighbours(below, above, second)
    summed = summed_chunks(own, others, jnp.asarray(order.T, jnp.bfloat16), capacity)
    returned = far_exchange(summed)
    return mixed_layers(
        returned, ids, route, own_columns, past_layers, dwa_weight, experts, capacity
    )


def solution(mesh):
    return jax.shard_map(
        per_device,
        mesh=mesh,
        in_specs=(
            P(("expert", "dp"), None),
            P(("expert", "dp"), None),
            P(("expert", "dp"), None),
            P("expert", None, ("dp", "tensor")),
            P("expert", None, ("dp", "tensor")),
            P("expert", "dp", "tensor"),
            P(None, ("expert", "dp"), "tensor"),
            P(),
        ),
        out_specs=P(("expert", "dp"), "tensor"),
        check_vma=False,
    )
```

```python
import jax
import jax.numpy as jnp
import numpy as np
from jax import lax
from jax.experimental import pallas as pl
from jax.experimental.pallas import tpu as pltpu
from jax.sharding import PartitionSpec as P

RADIX = 4
LANES = 128
TERMS = 3
SHIFTS = (0, 1, 3, 2)
LIMIT = pltpu.CompilerParams(vmem_limit_bytes=16 * 2**20)
HBM = pl.BlockSpec(memory_space=pltpu.HBM)
SMEM = pl.BlockSpec(memory_space=pltpu.SMEM)
VMEM = pl.BlockSpec(memory_space=pltpu.VMEM)


def in_hbm(array):
    return pltpu.with_memory_space_constraint(array, pltpu.HBM)


def far_groups():
    experts, count = lax.axis_size("expert"), lax.axis_size("dp")
    stride = count // RADIX
    return [
        [expert * count + low + stride * high for expert in range(experts) for high in range(RADIX)]
        for low in range(stride)
    ]


def far_exchange(chunks):
    return lax.all_to_all(chunks, ("expert", "dp"), 0, 0, tiled=True, axis_index_groups=far_groups())


def shifted(shard, even_shift, odd_shift):
    experts, count = lax.axis_size("expert"), lax.axis_size("dp")
    pairs = []
    for expert in range(experts):
        shift = odd_shift if expert % 2 else even_shift
        for place in range(count):
            pairs.append((expert * count + place, expert * count + (place + shift) % count))
    return lax.ppermute(shard, ("expert", "dp"), pairs)


def from_neighbours(shard):
    return [shifted(shard, 1, 1), shifted(shard, -1, -1), shifted(shard, 2, -2)]


def to_neighbours(shards):
    below, above, second = shards
    return [shifted(below, -1, -1), shifted(above, 1, 1), shifted(second, -2, 2)]


def call(kernel, name, out_shape, *operands, in_specs=None):
    many = isinstance(out_shape, list)
    return pl.pallas_call(
        kernel,
        out_shape=out_shape,
        in_specs=in_specs or [VMEM] * len(operands),
        out_specs=[VMEM] * len(out_shape) if many else VMEM,
        compiler_params=LIMIT,
        name=name,
    )(*operands)


def repeated_ids(ids):
    tok_rows = ids.shape[1]
    token = lax.broadcasted_iota(jnp.int32, (tok_rows, LANES), 0)
    lane = lax.broadcasted_iota(jnp.int32, (tok_rows, LANES), 1)
    spread = (lane % tok_rows == token).astype(jnp.float32)
    return jnp.dot(ids.astype(jnp.float32), spread, preferred_element_type=jnp.float32)


def assigned_slots(ids, experts, tok_rows):
    ids = repeated_ids(ids)
    choices, lanes = ids.shape
    expert = lax.broadcasted_iota(jnp.int32, (experts, lanes), 0).astype(jnp.float32)
    chosen = [ids[place : place + 1, :] == expert for place in range(choices)]
    named = sum(mask.astype(jnp.float32) for mask in chosen)
    source = lax.broadcasted_iota(jnp.int32, (lanes, lanes), 0)
    token = lax.broadcasted_iota(jnp.int32, (lanes, lanes), 1) % tok_rows
    before = (source < token).astype(jnp.float32)
    earlier = jnp.dot(named, before, preferred_element_type=jnp.float32)
    return [jnp.where(mask, earlier, -1.0) for mask in chosen]


def placed(slots, values, capacity, tok_rows):
    experts, lanes = slots[0].shape
    blocks = lanes // tok_rows
    shape = (capacity * blocks, lanes)
    row = lax.broadcasted_iota(jnp.int32, shape, 0)
    column = lax.broadcasted_iota(jnp.int32, shape, 1)
    same_block = row % blocks == column // tok_rows
    slot = (row // blocks).astype(jnp.float32)
    pieces = []
    for expert in range(experts):
        piece = jnp.zeros(shape, jnp.float32)
        for found, value in zip(slots, values):
            piece += jnp.where(same_block & (found[expert : expert + 1, :] == slot), value, 0.0)
        pieces.append(piece)
    return jnp.concatenate(pieces, axis=0)


def packed_rows(ids, tokens, first_column, quarter, experts, capacity):
    tok_rows = tokens.shape[0]
    blocks = quarter // LANES

    def kernel(first_ref, ids_in_ref, tokens_ref, out_ref, own_ref, ids_ref, named, arrived):
        first = pl.multiple_of(first_ref[0], LANES)
        ids_copy = pltpu.make_async_copy(ids_in_ref, ids_ref, named)
        copy = pltpu.make_async_copy(tokens_ref.at[:, pl.ds(first, quarter)], own_ref, arrived)
        ids_copy.start()
        copy.start()
        ids_copy.wait()
        slots = assigned_slots(ids_ref[...], experts, tok_rows)
        chosen = placed(slots, [1.0] * len(slots), capacity, tok_rows).astype(jnp.bfloat16)
        copy.wait()
        tall = [own_ref[:, block * LANES : (block + 1) * LANES] for block in range(blocks)]
        out = jnp.dot(chosen, jnp.concatenate(tall, axis=0), preferred_element_type=jnp.float32)
        out = out.astype(out_ref.dtype)
        height = capacity * blocks
        for expert in range(experts):
            for far in range(RADIX):
                out_ref[expert * RADIX + far] = out[expert * height : (expert + 1) * height]

    return pl.pallas_call(
        kernel,
        out_shape=[
            jax.ShapeDtypeStruct((experts * RADIX, capacity * blocks, LANES), tokens.dtype),
            jax.ShapeDtypeStruct((tok_rows, quarter), tokens.dtype),
        ],
        in_specs=[SMEM, HBM, HBM],
        out_specs=[VMEM, VMEM],
        scratch_shapes=[pltpu.VMEM(ids.shape, ids.dtype), pltpu.SemaphoreType.DMA, pltpu.SemaphoreType.DMA],
        compiler_params=LIMIT,
        name="packed_rows",
    )(first_column, ids, tokens)


def chunk_order(chunks, capacity, blocks):
    count = chunks * capacity * blocks
    order = np.arange(count).reshape(chunks, capacity, blocks).transpose(2, 0, 1).reshape(-1)
    return np.eye(count, dtype=np.float32)[order]


def wide_rows(chunks, order, capacity):
    count, height, _ = chunks.shape
    blocks = height // capacity
    together = order.shape[0] // height
    rows = together * capacity

    def kernel(order_ref, in_ref, out_ref):
        for group in range(count // together):
            tall = in_ref[group * together : (group + 1) * together].reshape(together * height, LANES)
            out = jnp.dot(order_ref[...], tall, preferred_element_type=jnp.float32).astype(out_ref.dtype)
            for block in range(blocks):
                piece = out[block * rows : (block + 1) * rows]
                out_ref[group * rows : (group + 1) * rows, block * LANES : (block + 1) * LANES] = piece

    shape = jax.ShapeDtypeStruct((count * capacity, blocks * LANES), chunks.dtype)
    return call(kernel, "wide_rows", shape, order, chunks)


def summed_chunks(own, others, order, capacity):
    total_rows, features = own.shape
    blocks = features // LANES
    height = capacity * blocks
    together = order.shape[0] // height
    rows = together * capacity

    def kernel(order_ref, own_ref, *refs):
        other_refs, out_ref = refs[:-1], refs[-1]
        total = own_ref[...]
        for ref in other_refs:
            total += ref[...].astype(jnp.float32)
        total = total.astype(out_ref.dtype)
        for group in range(total_rows // rows):
            part = total[group * rows : (group + 1) * rows]
            tall = [part[:, block * LANES : (block + 1) * LANES] for block in range(blocks)]
            out = jnp.dot(order_ref[...], jnp.concatenate(tall, axis=0), preferred_element_type=jnp.float32)
            out = out.astype(out_ref.dtype).reshape(together, height, LANES)
            out_ref[group * together : (group + 1) * together] = out

    shape = jax.ShapeDtypeStruct((total_rows // capacity, height, LANES), jnp.bfloat16)
    return call(kernel, "summed_chunks", shape, order, own, *others)


def weights_by_features(gate_weight, up_weight, quarter):
    parts = lax.axis_size("tensor")
    here = lax.axis_index("tensor")
    slabs = [w.reshape(parts, quarter, -1) for w in (gate_weight, up_weight)]

    def slab(shift):
        place = (here + shift) % parts
        both = [lax.dynamic_index_in_dim(w, place, 0, keepdims=False) for w in slabs]
        both = jnp.concatenate(both, axis=1)
        if shift == 0:
            return both
        return lax.ppermute(both, "tensor", [(i, (i + shift) % parts) for i in range(parts)])

    return [slab(shift) for shift in SHIFTS]


def gate_up_parts(sets, weights, place):
    parts = len(weights)
    width = weights[0].shape[1]
    set_rows = sets[0].shape[0]
    rows = set_rows * len(sets)

    def kernel(place_ref, *refs):
        set_refs, w_refs, out_ref = refs[: len(sets)], refs[len(sets) : -1], refs[-1]
        stacked = jnp.concatenate([ref[...] for ref in set_refs], axis=0)
        for shift, w_ref in zip(SHIFTS, w_refs):
            part = (place_ref[0] + (parts - shift)) % parts
            out = jnp.dot(stacked, w_ref[...], preferred_element_type=jnp.float32)
            out_ref[part] = out.astype(out_ref.dtype)

    shape = jax.ShapeDtypeStruct((parts, rows, width), jnp.bfloat16)
    specs = [SMEM] + [VMEM] * (len(sets) + parts)
    return call(kernel, "gate_up_parts", shape, place, *sets, *weights, in_specs=specs)


def hidden_units(parts):
    count, rows, both = parts.shape
    width = both // 2

    def kernel(in_ref, out_ref):
        total = in_ref[0].astype(jnp.float32)
        for part in range(1, count):
            total += in_ref[part].astype(jnp.float32)
        gate, up = total[:, :width], total[:, width:]
        out_ref[...] = (gate / (1.0 + jnp.exp(-gate)) * up).astype(out_ref.dtype)

    return call(kernel, "hidden_units", jax.ShapeDtypeStruct((rows, width), jnp.bfloat16), parts)


def down_sets(hidden, w_down, count):
    parts, rows, _ = hidden.shape
    set_rows = rows // count
    features = w_down.shape[1]

    def kernel(hidden_ref, w_ref, *out_refs):
        wide = jnp.concatenate([hidden_ref[part] for part in range(parts)], axis=1)
        out = jnp.dot(wide, w_ref[...], preferred_element_type=jnp.float32)
        for place, ref in enumerate(out_refs):
            ref[...] = out[place * set_rows : (place + 1) * set_rows].astype(ref.dtype)

    shapes = [
        jax.ShapeDtypeStruct((set_rows, features), jnp.bfloat16 if place else jnp.float32)
        for place in range(count)
    ]
    return call(kernel, "down_sets", shapes, hidden, w_down)


def mix_terms(ids, route, own_columns, past_layers, dwa_weight, experts, capacity):
    tok_rows, features = own_columns.shape
    height = capacity * (features // LANES)
    depth = past_layers.shape[0]

    def kernel(dwa_ref, ids_ref, route_ref, own_ref, past_ref, terms_ref, base_ref):
        slots = assigned_slots(ids_ref[...], experts, tok_rows)
        route = route_ref[...]
        total = sum(route[place : place + 1, :] for place in range(len(slots)))
        shares = [dwa_ref[depth] * (route[place : place + 1, :] / total) for place in range(len(slots))]
        rest = placed(slots, shares, capacity, tok_rows)
        for place in range(TERMS):
            term = rest.astype(jnp.bfloat16)
            rest = rest - term.astype(jnp.float32)
            terms_ref[place] = term
        base = dwa_ref[depth] * own_ref[...].astype(jnp.float32)
        for layer in range(depth):
            base += dwa_ref[layer] * past_ref[layer].astype(jnp.float32)
        base_ref[...] = base

    shapes = [
        jax.ShapeDtypeStruct((TERMS, experts * height, LANES), jnp.bfloat16),
        jax.ShapeDtypeStruct((tok_rows, features), jnp.float32),
    ]
    operands = (dwa_weight, ids, route, own_columns, past_layers)
    return call(kernel, "mix_terms", shapes, *operands, in_specs=[SMEM] + [VMEM] * 4)


def mixed_layers(returned, terms, base, dtype):
    tok_rows, features = base.shape
    experts = returned.shape[0] // RADIX

    def kernel(terms_ref, base_ref, in_ref, out_ref):
        outs = []
        for expert in range(experts):
            total = in_ref[expert * RADIX].astype(jnp.float32)
            for far in range(1, RADIX):
                total += in_ref[expert * RADIX + far].astype(jnp.float32)
            outs.append(total.astype(jnp.bfloat16))
        outs = jnp.concatenate(outs, axis=0)
        mix = jnp.zeros((features // LANES * tok_rows, LANES), jnp.float32)
        for place in range(TERMS):
            mix += lax.dot_general(
                terms_ref[place], outs, (((0,), (0,)), ((), ())), preferred_element_type=jnp.float32
            )
        for block in range(features // LANES):
            lanes = slice(block * LANES, (block + 1) * LANES)
            value = base_ref[:, lanes] + mix[block * tok_rows : (block + 1) * tok_rows]
            out_ref[:, lanes] = value.astype(out_ref.dtype)

    shape = jax.ShapeDtypeStruct((tok_rows, features), dtype)
    return call(kernel, "mixed_layers", shape, terms, base, returned)


def per_device(
    tokens, expert_ids, route_weight, gate_weight, up_weight, down_weight, past_layers, dwa_weight
):
    experts = lax.axis_size("expert")
    parts = lax.axis_size("tensor")
    tok_rows, feature_width = tokens.shape
    chosen_count = expert_ids.shape[1]
    capacity = min(tok_rows, 3 * chosen_count * tok_rows // (2 * experts))
    quarter = feature_width // parts
    blocks = quarter // LANES
    together = 2 * RADIX
    order = chunk_order(together, capacity, blocks)
    ids = expert_ids.T
    route = jnp.tile(route_weight.T, (1, blocks))
    weights = weights_by_features(gate_weight, up_weight, quarter)
    place = lax.axis_index("tensor").reshape(1)
    packed, own_columns = packed_rows(in_hbm(ids), in_hbm(tokens), place * quarter, quarter, experts, capacity)
    arrived = far_exchange(packed)
    own_set = wide_rows(arrived, jnp.asarray(order, jnp.bfloat16), capacity)
    sets = [own_set, *from_neighbours(own_set)]
    partial = lax.all_to_all(gate_up_parts(sets, weights, place), "tensor", 0, 0, tiled=True)
    hidden = lax.all_gather(hidden_units(partial), "tensor", axis=0, tiled=False)
    own, *others = down_sets(hidden, down_weight[0], len(sets))
    route, own = lax.optimization_barrier((route, own))
    terms, base = mix_terms(ids, route, own_columns, past_layers, dwa_weight, experts, capacity)
    others = to_neighbours(others)
    own, terms, base = lax.optimization_barrier((own, terms, base))
    returned = far_exchange(summed_chunks(own, others, jnp.asarray(order.T, jnp.bfloat16), capacity))
    return mixed_layers(returned, terms, base, tokens.dtype)


def solution(mesh):
    return jax.shard_map(
        per_device,
        mesh=mesh,
        in_specs=(
            P(("expert", "dp"), None),
            P(("expert", "dp"), None),
            P(("expert", "dp"), None),
            P("expert", None, ("dp", "tensor")),
            P("expert", None, ("dp", "tensor")),
            P("expert", "dp", "tensor"),
            P(None, ("expert", "dp"), "tensor"),
            P(),
        ),
        out_specs=P(("expert", "dp"), "tensor"),
        check_vma=False,
    )
```

```python
import jax
import jax.numpy as jnp
import numpy as np
from jax import lax
from jax.experimental import pallas as pl
from jax.experimental.pallas import tpu as pltpu
from jax.sharding import PartitionSpec as P

RADIX = 4
LANES = 128
TERMS = 3
SHIFTS = (0, 1, 3, 2)
LIMIT = pltpu.CompilerParams(vmem_limit_bytes=16 * 2**20)
HBM = pl.BlockSpec(memory_space=pltpu.HBM)
SMEM = pl.BlockSpec(memory_space=pltpu.SMEM)
VMEM = pl.BlockSpec(memory_space=pltpu.VMEM)


def in_hbm(array):
    return pltpu.with_memory_space_constraint(array, pltpu.HBM)


def far_groups():
    experts, count = lax.axis_size("expert"), lax.axis_size("dp")
    stride = count // RADIX
    return [
        [expert * count + low + stride * high for expert in range(experts) for high in range(RADIX)]
        for low in range(stride)
    ]


def far_exchange(chunks):
    return lax.all_to_all(chunks, ("expert", "dp"), 0, 0, tiled=True, axis_index_groups=far_groups())


def shifted(shard, even_shift, odd_shift):
    experts, count = lax.axis_size("expert"), lax.axis_size("dp")
    pairs = []
    for expert in range(experts):
        shift = odd_shift if expert % 2 else even_shift
        for place in range(count):
            pairs.append((expert * count + place, expert * count + (place + shift) % count))
    return lax.ppermute(shard, ("expert", "dp"), pairs)


def forward(shard):
    return shifted(shard, 1, -1)


def backward(shard):
    return shifted(shard, -1, 1)


def window_sets(own):
    first, other = forward(own), backward(own)
    return [own, first, other, forward(first)]


def returned_sums(first, other, second):
    relayed = backward(second)
    other = forward(other)
    first = (first + relayed.astype(jnp.float32)).astype(jnp.bfloat16)
    return [backward(first), other]


def call(kernel, out_shape, *operands, in_specs=None):
    many = isinstance(out_shape, list)
    return pl.pallas_call(
        kernel,
        out_shape=out_shape,
        in_specs=in_specs or [VMEM] * len(operands),
        out_specs=[VMEM] * len(out_shape) if many else VMEM,
        compiler_params=LIMIT,
    )(*operands)


def repeated_ids(ids):
    tok_rows = ids.shape[1]
    token = lax.broadcasted_iota(jnp.int32, (tok_rows, LANES), 0)
    lane = lax.broadcasted_iota(jnp.int32, (tok_rows, LANES), 1)
    spread = (lane % tok_rows == token).astype(jnp.float32)
    return jnp.dot(ids.astype(jnp.float32), spread, preferred_element_type=jnp.float32)


def assigned_slots(ids, experts, tok_rows):
    ids = repeated_ids(ids)
    choices, lanes = ids.shape
    expert = lax.broadcasted_iota(jnp.int32, (experts, lanes), 0).astype(jnp.float32)
    chosen = [ids[place : place + 1, :] == expert for place in range(choices)]
    named = sum(mask.astype(jnp.float32) for mask in chosen)
    source = lax.broadcasted_iota(jnp.int32, (lanes, lanes), 0)
    token = lax.broadcasted_iota(jnp.int32, (lanes, lanes), 1) % tok_rows
    before = (source < token).astype(jnp.float32)
    earlier = jnp.dot(named, before, preferred_element_type=jnp.float32)
    return [jnp.where(mask, earlier, -1.0) for mask in chosen]


def placed(slots, values, capacity, tok_rows):
    experts, lanes = slots[0].shape
    blocks = lanes // tok_rows
    shape = (capacity * blocks, lanes)
    row = lax.broadcasted_iota(jnp.int32, shape, 0)
    column = lax.broadcasted_iota(jnp.int32, shape, 1)
    same_block = row % blocks == column // tok_rows
    slot = (row // blocks).astype(jnp.float32)
    pieces = []
    for expert in range(experts):
        piece = jnp.zeros(shape, jnp.float32)
        for found, value in zip(slots, values):
            piece += jnp.where(same_block & (found[expert : expert + 1, :] == slot), value, 0.0)
        pieces.append(piece)
    return jnp.concatenate(pieces, axis=0)


def packed_rows(ids, tokens, first_column, quarter, experts, capacity):
    tok_rows = tokens.shape[0]
    blocks = quarter // LANES

    def kernel(first_ref, ids_in_ref, tokens_ref, out_ref, own_ref, ids_ref, named, arrived):
        first = pl.multiple_of(first_ref[0], LANES)
        ids_copy = pltpu.make_async_copy(ids_in_ref, ids_ref, named)
        copy = pltpu.make_async_copy(tokens_ref.at[:, pl.ds(first, quarter)], own_ref, arrived)
        ids_copy.start()
        copy.start()
        ids_copy.wait()
        slots = assigned_slots(ids_ref[...], experts, tok_rows)
        chosen = placed(slots, [1.0] * len(slots), capacity, tok_rows).astype(jnp.bfloat16)
        copy.wait()
        tall = [own_ref[:, block * LANES : (block + 1) * LANES] for block in range(blocks)]
        out = jnp.dot(chosen, jnp.concatenate(tall, axis=0), preferred_element_type=jnp.float32)
        out = out.astype(out_ref.dtype)
        height = capacity * blocks
        for expert in range(experts):
            for far in range(RADIX):
                out_ref[expert * RADIX + far] = out[expert * height : (expert + 1) * height]

    return pl.pallas_call(
        kernel,
        out_shape=[
            jax.ShapeDtypeStruct((experts * RADIX, capacity * blocks, LANES), tokens.dtype),
            jax.ShapeDtypeStruct((tok_rows, quarter), tokens.dtype),
        ],
        in_specs=[SMEM, HBM, HBM],
        out_specs=[VMEM, VMEM],
        scratch_shapes=[pltpu.VMEM(ids.shape, ids.dtype), pltpu.SemaphoreType.DMA, pltpu.SemaphoreType.DMA],
        compiler_params=LIMIT,
        name="packed_rows",
    )(first_column, ids, tokens)


def chunk_order(chunks, capacity, blocks):
    count = chunks * capacity * blocks
    order = np.arange(count).reshape(chunks, capacity, blocks).transpose(2, 0, 1).reshape(-1)
    return np.eye(count, dtype=np.float32)[order]


def wide_rows(chunks, order, capacity):
    count, height, _ = chunks.shape
    blocks = height // capacity
    together = order.shape[0] // height
    rows = together * capacity

    def kernel(order_ref, in_ref, out_ref):
        for group in range(count // together):
            tall = in_ref[group * together : (group + 1) * together].reshape(together * height, LANES)
            out = jnp.dot(order_ref[...], tall, preferred_element_type=jnp.float32).astype(out_ref.dtype)
            for block in range(blocks):
                piece = out[block * rows : (block + 1) * rows]
                out_ref[group * rows : (group + 1) * rows, block * LANES : (block + 1) * LANES] = piece

    shape = jax.ShapeDtypeStruct((count * capacity, blocks * LANES), chunks.dtype)
    return call(kernel, shape, order, chunks)


def summed_chunks(own, others, order, capacity):
    total_rows, features = own.shape
    blocks = features // LANES
    height = capacity * blocks
    together = order.shape[0] // height
    rows = together * capacity

    def kernel(order_ref, own_ref, *refs):
        other_refs, out_ref = refs[:-1], refs[-1]
        total = own_ref[...]
        for ref in other_refs:
            total += ref[...].astype(jnp.float32)
        total = total.astype(out_ref.dtype)
        for group in range(total_rows // rows):
            part = total[group * rows : (group + 1) * rows]
            tall = [part[:, block * LANES : (block + 1) * LANES] for block in range(blocks)]
            out = jnp.dot(order_ref[...], jnp.concatenate(tall, axis=0), preferred_element_type=jnp.float32)
            out = out.astype(out_ref.dtype).reshape(together, height, LANES)
            out_ref[group * together : (group + 1) * together] = out

    shape = jax.ShapeDtypeStruct((total_rows // capacity, height, LANES), jnp.bfloat16)
    return call(kernel, shape, order, own, *others)


def weights_by_features(gate_weight, up_weight, quarter):
    parts = lax.axis_size("tensor")
    here = lax.axis_index("tensor")
    slabs = [w.reshape(parts, quarter, -1) for w in (gate_weight, up_weight)]

    def slab(shift):
        place = (here + shift) % parts
        both = [lax.dynamic_index_in_dim(w, place, 0, keepdims=False) for w in slabs]
        both = jnp.concatenate(both, axis=1)
        if shift == 0:
            return both
        return lax.ppermute(both, "tensor", [(i, (i + shift) % parts) for i in range(parts)])

    return [slab(shift) for shift in SHIFTS]


def gate_up_parts(sets, weights, place):
    parts = len(weights)
    width = weights[0].shape[1]
    set_rows = sets[0].shape[0]
    rows = set_rows * len(sets)

    def kernel(place_ref, *refs):
        set_refs, w_refs, out_ref = refs[: len(sets)], refs[len(sets) : -1], refs[-1]
        stacked = jnp.concatenate([ref[...] for ref in set_refs], axis=0)
        for shift, w_ref in zip(SHIFTS, w_refs):
            part = (place_ref[0] + (parts - shift)) % parts
            out = jnp.dot(stacked, w_ref[...], preferred_element_type=jnp.float32)
            out_ref[part] = out.astype(out_ref.dtype)

    shape = jax.ShapeDtypeStruct((parts, rows, width), jnp.bfloat16)
    specs = [SMEM] + [VMEM] * (len(sets) + parts)
    return call(kernel, shape, place, *sets, *weights, in_specs=specs)


def hidden_units(parts):
    count, rows, both = parts.shape
    width = both // 2

    def kernel(in_ref, out_ref):
        total = in_ref[0].astype(jnp.float32)
        for part in range(1, count):
            total += in_ref[part].astype(jnp.float32)
        gate, up = total[:, :width], total[:, width:]
        out_ref[...] = (gate / (1.0 + jnp.exp(-gate)) * up).astype(out_ref.dtype)

    return call(kernel, jax.ShapeDtypeStruct((rows, width), jnp.bfloat16), parts)


def down_sets(hidden, w_down, dtypes):
    parts, rows, _ = hidden.shape
    set_rows = rows // len(dtypes)
    features = w_down.shape[1]

    def kernel(hidden_ref, w_ref, *out_refs):
        wide = jnp.concatenate([hidden_ref[part] for part in range(parts)], axis=1)
        out = jnp.dot(wide, w_ref[...], preferred_element_type=jnp.float32)
        for place, ref in enumerate(out_refs):
            ref[...] = out[place * set_rows : (place + 1) * set_rows].astype(ref.dtype)

    shapes = [jax.ShapeDtypeStruct((set_rows, features), dtype) for dtype in dtypes]
    return call(kernel, shapes, hidden, w_down)


def mix_terms(ids, route, own_columns, past_layers, dwa_weight, experts, capacity):
    tok_rows, features = own_columns.shape
    height = capacity * (features // LANES)
    depth = past_layers.shape[0]

    def kernel(dwa_ref, ids_ref, route_ref, own_ref, past_ref, terms_ref, base_ref):
        slots = assigned_slots(ids_ref[...], experts, tok_rows)
        route = route_ref[...]
        total = sum(route[place : place + 1, :] for place in range(len(slots)))
        shares = [dwa_ref[depth] * (route[place : place + 1, :] / total) for place in range(len(slots))]
        rest = placed(slots, shares, capacity, tok_rows)
        for place in range(TERMS):
            term = rest.astype(jnp.bfloat16)
            rest = rest - term.astype(jnp.float32)
            terms_ref[place] = term
        base = dwa_ref[depth] * own_ref[...].astype(jnp.float32)
        for layer in range(depth):
            base += dwa_ref[layer] * past_ref[layer].astype(jnp.float32)
        base_ref[...] = base

    shapes = [
        jax.ShapeDtypeStruct((TERMS, experts * height, LANES), jnp.bfloat16),
        jax.ShapeDtypeStruct((tok_rows, features), jnp.float32),
    ]
    operands = (dwa_weight, ids, route, own_columns, past_layers)
    return call(kernel, shapes, *operands, in_specs=[SMEM] + [VMEM] * 4)


def mixed_layers(returned, terms, base, dtype):
    tok_rows, features = base.shape
    experts = returned.shape[0] // RADIX

    def kernel(terms_ref, base_ref, in_ref, out_ref):
        outs = []
        for expert in range(experts):
            total = in_ref[expert * RADIX].astype(jnp.float32)
            for far in range(1, RADIX):
                total += in_ref[expert * RADIX + far].astype(jnp.float32)
            outs.append(total.astype(jnp.bfloat16))
        outs = jnp.concatenate(outs, axis=0)
        mix = jnp.zeros((features // LANES * tok_rows, LANES), jnp.float32)
        for place in range(TERMS):
            mix += lax.dot_general(
                terms_ref[place], outs, (((0,), (0,)), ((), ())), preferred_element_type=jnp.float32
            )
        for block in range(features // LANES):
            lanes = slice(block * LANES, (block + 1) * LANES)
            value = base_ref[:, lanes] + mix[block * tok_rows : (block + 1) * tok_rows]
            out_ref[:, lanes] = value.astype(out_ref.dtype)

    shape = jax.ShapeDtypeStruct((tok_rows, features), dtype)
    return call(kernel, shape, terms, base, returned)


def per_device(
    tokens, expert_ids, route_weight, gate_weight, up_weight, down_weight, past_layers, dwa_weight
):
    experts = lax.axis_size("expert")
    parts = lax.axis_size("tensor")
    tok_rows, feature_width = tokens.shape
    chosen_count = expert_ids.shape[1]
    capacity = min(tok_rows, 3 * chosen_count * tok_rows // (2 * experts))
    quarter = feature_width // parts
    blocks = quarter // LANES
    together = 2 * RADIX
    order = chunk_order(together, capacity, blocks)
    ids = expert_ids.T
    route = jnp.tile(route_weight.T, (1, blocks))
    weights = weights_by_features(gate_weight, up_weight, quarter)
    place = lax.axis_index("tensor").reshape(1)
    packed, own_columns = packed_rows(in_hbm(ids), in_hbm(tokens), place * quarter, quarter, experts, capacity)
    arrived = far_exchange(packed)
    own_set = wide_rows(arrived, jnp.asarray(order, jnp.bfloat16), capacity)
    sets = window_sets(own_set)
    partial = lax.all_to_all(gate_up_parts(sets, weights, place), "tensor", 0, 0, tiled=True)
    hidden = lax.all_gather(hidden_units(partial), "tensor", axis=0, tiled=False)
    own, *others = down_sets(hidden, down_weight[0], [jnp.float32] * 2 + [jnp.bfloat16] * 2)
    route, own = lax.optimization_barrier((route, own))
    terms, base = mix_terms(ids, route, own_columns, past_layers, dwa_weight, experts, capacity)
    others = returned_sums(*others)
    own, terms, base = lax.optimization_barrier((own, terms, base))
    returned = far_exchange(summed_chunks(own, others, jnp.asarray(order.T, jnp.bfloat16), capacity))
    return mixed_layers(returned, terms, base, tokens.dtype)


def solution(mesh):
    return jax.shard_map(
        per_device,
        mesh=mesh,
        in_specs=(
            P(("expert", "dp"), None),
            P(("expert", "dp"), None),
            P(("expert", "dp"), None),
            P("expert", None, ("dp", "tensor")),
            P("expert", None, ("dp", "tensor")),
            P("expert", "dp", "tensor"),
            P(None, ("expert", "dp"), "tensor"),
            P(),
        ),
        out_specs=P(("expert", "dp"), "tensor"),
        check_vma=False,
    )
```

```python
import jax
import jax.numpy as jnp
import numpy as np
from jax import lax
from jax.experimental import pallas as pl
from jax.experimental.pallas import tpu as pltpu
from jax.sharding import PartitionSpec as P

RADIX = 4
LANES = 128
TERMS = 3
LIMIT = pltpu.CompilerParams(vmem_limit_bytes=16 * 2**20)
HBM = pl.BlockSpec(memory_space=pltpu.HBM)
SMEM = pl.BlockSpec(memory_space=pltpu.SMEM)
VMEM = pl.BlockSpec(memory_space=pltpu.VMEM)


def in_hbm(array):
    return pltpu.with_memory_space_constraint(array, pltpu.HBM)


def far_groups():
    experts, count = lax.axis_size("expert"), lax.axis_size("dp")
    stride = count // RADIX
    return [
        [expert * count + low + stride * high for expert in range(experts) for high in range(RADIX)]
        for low in range(stride)
    ]


def far_exchange(chunks):
    return lax.all_to_all(chunks, ("expert", "dp"), 0, 0, tiled=True, axis_index_groups=far_groups())


def shifted(shard, even_shift, odd_shift):
    experts, count = lax.axis_size("expert"), lax.axis_size("dp")
    pairs = []
    for expert in range(experts):
        shift = odd_shift if expert % 2 else even_shift
        for place in range(count):
            pairs.append((expert * count + place, expert * count + (place + shift) % count))
    return lax.ppermute(shard, ("expert", "dp"), pairs)


def forward(shard):
    return shifted(shard, 1, -1)


def backward(shard):
    return shifted(shard, -1, 1)


def window_sets(own):
    first, other = forward(own), backward(own)
    return [own, first, other, forward(first)]


def returned_sums(first, other, second):
    relayed = backward(second)
    other = forward(other)
    first = (first + relayed.astype(jnp.float32)).astype(jnp.bfloat16)
    return [backward(first), other]


def call(kernel, out_shape, *operands, in_specs=None):
    many = isinstance(out_shape, list)
    return pl.pallas_call(
        kernel,
        out_shape=out_shape,
        in_specs=in_specs or [VMEM] * len(operands),
        out_specs=[VMEM] * len(out_shape) if many else VMEM,
        compiler_params=LIMIT,
    )(*operands)


def repeated_ids(ids):
    tok_rows = ids.shape[1]
    token = lax.broadcasted_iota(jnp.int32, (tok_rows, LANES), 0)
    lane = lax.broadcasted_iota(jnp.int32, (tok_rows, LANES), 1)
    spread = (lane % tok_rows == token).astype(jnp.float32)
    return jnp.dot(ids.astype(jnp.float32), spread, preferred_element_type=jnp.float32)


def assigned_slots(ids, experts, tok_rows):
    ids = repeated_ids(ids)
    choices, lanes = ids.shape
    expert = lax.broadcasted_iota(jnp.int32, (experts, lanes), 0).astype(jnp.float32)
    chosen = [ids[place : place + 1, :] == expert for place in range(choices)]
    named = sum(mask.astype(jnp.float32) for mask in chosen)
    source = lax.broadcasted_iota(jnp.int32, (lanes, lanes), 0)
    token = lax.broadcasted_iota(jnp.int32, (lanes, lanes), 1) % tok_rows
    before = (source < token).astype(jnp.float32)
    earlier = jnp.dot(named, before, preferred_element_type=jnp.float32)
    return [jnp.where(mask, earlier, -1.0) for mask in chosen]


def placed(slots, values, capacity, tok_rows):
    experts, lanes = slots[0].shape
    blocks = lanes // tok_rows
    shape = (capacity * blocks, lanes)
    row = lax.broadcasted_iota(jnp.int32, shape, 0)
    column = lax.broadcasted_iota(jnp.int32, shape, 1)
    same_block = row % blocks == column // tok_rows
    slot = (row // blocks).astype(jnp.float32)
    pieces = []
    for expert in range(experts):
        piece = jnp.zeros(shape, jnp.float32)
        for found, value in zip(slots, values):
            piece += jnp.where(same_block & (found[expert : expert + 1, :] == slot), value, 0.0)
        pieces.append(piece)
    return jnp.concatenate(pieces, axis=0)


def packed_rows(ids, tokens, first_column, quarter, experts, capacity):
    tok_rows = tokens.shape[0]
    blocks = quarter // LANES

    def kernel(first_ref, ids_in_ref, tokens_ref, out_ref, own_ref, ids_ref, named, arrived):
        first = pl.multiple_of(first_ref[0], LANES)
        ids_copy = pltpu.make_async_copy(ids_in_ref, ids_ref, named)
        copy = pltpu.make_async_copy(tokens_ref.at[:, pl.ds(first, quarter)], own_ref, arrived)
        ids_copy.start()
        copy.start()
        ids_copy.wait()
        slots = assigned_slots(ids_ref[...], experts, tok_rows)
        chosen = placed(slots, [1.0] * len(slots), capacity, tok_rows).astype(jnp.bfloat16)
        copy.wait()
        tall = [own_ref[:, block * LANES : (block + 1) * LANES] for block in range(blocks)]
        out = jnp.dot(chosen, jnp.concatenate(tall, axis=0), preferred_element_type=jnp.float32)
        out = out.astype(out_ref.dtype)
        height = capacity * blocks
        for expert in range(experts):
            for far in range(RADIX):
                out_ref[expert * RADIX + far] = out[expert * height : (expert + 1) * height]

    return pl.pallas_call(
        kernel,
        out_shape=[
            jax.ShapeDtypeStruct((experts * RADIX, capacity * blocks, LANES), tokens.dtype),
            jax.ShapeDtypeStruct((tok_rows, quarter), tokens.dtype),
        ],
        in_specs=[SMEM, HBM, HBM],
        out_specs=[VMEM, VMEM],
        scratch_shapes=[pltpu.VMEM(ids.shape, ids.dtype), pltpu.SemaphoreType.DMA, pltpu.SemaphoreType.DMA],
        compiler_params=LIMIT,
        name="packed_rows",
    )(first_column, ids, tokens)


def chunk_order(chunks, capacity, blocks):
    count = chunks * capacity * blocks
    order = np.arange(count).reshape(chunks, capacity, blocks).transpose(2, 0, 1).reshape(-1)
    return np.eye(count, dtype=np.float32)[order]


def wide_rows(chunks, order, capacity):
    count, height, _ = chunks.shape
    blocks = height // capacity
    together = order.shape[0] // height
    rows = together * capacity

    def kernel(order_ref, in_ref, out_ref):
        for group in range(count // together):
            tall = in_ref[group * together : (group + 1) * together].reshape(together * height, LANES)
            out = jnp.dot(order_ref[...], tall, preferred_element_type=jnp.float32).astype(out_ref.dtype)
            for block in range(blocks):
                piece = out[block * rows : (block + 1) * rows]
                out_ref[group * rows : (group + 1) * rows, block * LANES : (block + 1) * LANES] = piece

    shape = jax.ShapeDtypeStruct((count * capacity, blocks * LANES), chunks.dtype)
    return call(kernel, shape, order, chunks)


def summed_chunks(own, others, order, capacity):
    total_rows, features = own.shape
    blocks = features // LANES
    height = capacity * blocks
    together = order.shape[0] // height
    rows = together * capacity

    def kernel(order_ref, own_ref, *refs):
        other_refs, out_ref = refs[:-1], refs[-1]
        total = own_ref[...]
        for ref in other_refs:
            total += ref[...].astype(jnp.float32)
        total = total.astype(out_ref.dtype)
        for group in range(total_rows // rows):
            part = total[group * rows : (group + 1) * rows]
            tall = [part[:, block * LANES : (block + 1) * LANES] for block in range(blocks)]
            out = jnp.dot(order_ref[...], jnp.concatenate(tall, axis=0), preferred_element_type=jnp.float32)
            out = out.astype(out_ref.dtype).reshape(together, height, LANES)
            out_ref[group * together : (group + 1) * together] = out

    shape = jax.ShapeDtypeStruct((total_rows // capacity, height, LANES), jnp.bfloat16)
    return call(kernel, shape, order, own, *others)


def along_tensor(shard, even_shift, odd_shift):
    experts, count = lax.axis_size("expert"), lax.axis_size("tensor")
    pairs = []
    for expert in range(experts):
        shift = odd_shift if expert % 2 else even_shift
        for place in range(count):
            pairs.append((expert * count + place, expert * count + (place + shift) % count))
    return lax.ppermute(shard, ("expert", "tensor"), pairs)


def weights_by_features(gate_weight, up_weight, quarter):
    parts = lax.axis_size("tensor")
    here = lax.axis_index("tensor")
    step = jnp.where(lax.axis_index("expert") % 2 == 0, 1, parts - 1)
    slabs = [w.reshape(parts, quarter, -1) for w in (gate_weight, up_weight)]

    def slab(shift):
        place = (here + shift) % parts
        both = [lax.dynamic_index_in_dim(w, place, 0, keepdims=False) for w in slabs]
        return jnp.concatenate(both, axis=1)

    moves = [(parts - step, -1, 1), (step, 1, -1), (parts // 2, 2, 2)]
    weights = [slab(0)]
    for shift, even, odd in moves:
        weights.append(along_tensor(slab(shift), even, odd))
    return weights


def gate_up_parts(sets, weights):
    width = weights[0].shape[1]
    set_rows = sets[0].shape[0]
    rows = set_rows * len(sets)

    def kernel(*refs):
        set_refs, refs = refs[: len(sets)], refs[len(sets) :]
        w_refs, out_refs = refs[: len(weights)], refs[len(weights) :]
        stacked = jnp.concatenate([ref[...] for ref in set_refs], axis=0)
        for w_ref, out_ref in zip(w_refs, out_refs):
            out = jnp.dot(stacked, w_ref[...], preferred_element_type=jnp.float32)
            out_ref[...] = out.astype(out_ref.dtype)

    dtypes = [jnp.float32] * 2 + [jnp.bfloat16] * 2
    shapes = [jax.ShapeDtypeStruct((rows, width), dtype) for dtype in dtypes]
    return call(kernel, shapes, *sets, *weights)


def tensor_sums(following, previous, opposite):
    relayed = along_tensor(opposite, 1, -1)
    previous = along_tensor(previous, -1, 1)
    following = (following + relayed.astype(jnp.float32)).astype(jnp.bfloat16)
    return [along_tensor(following, 1, -1), previous]


def hidden_units(own, others):
    rows, both = own.shape
    width = both // 2

    def kernel(own_ref, *refs):
        other_refs, out_ref = refs[:-1], refs[-1]
        total = own_ref[...]
        for ref in other_refs:
            total += ref[...].astype(jnp.float32)
        gate, up = total[:, :width], total[:, width:]
        out_ref[...] = (gate / (1.0 + jnp.exp(-gate)) * up).astype(out_ref.dtype)

    shape = jax.ShapeDtypeStruct((rows, width), jnp.bfloat16)
    return call(kernel, shape, own, *others)


def down_sets(hidden, w_down, dtypes):
    parts, rows, _ = hidden.shape
    set_rows = rows // len(dtypes)
    features = w_down.shape[1]

    def kernel(hidden_ref, w_ref, *out_refs):
        wide = jnp.concatenate([hidden_ref[part] for part in range(parts)], axis=1)
        out = jnp.dot(wide, w_ref[...], preferred_element_type=jnp.float32)
        for place, ref in enumerate(out_refs):
            ref[...] = out[place * set_rows : (place + 1) * set_rows].astype(ref.dtype)

    shapes = [jax.ShapeDtypeStruct((set_rows, features), dtype) for dtype in dtypes]
    return call(kernel, shapes, hidden, w_down)


def mix_terms(ids, route, own_columns, past_layers, dwa_weight, experts, capacity):
    tok_rows, features = own_columns.shape
    height = capacity * (features // LANES)
    depth = past_layers.shape[0]

    def kernel(dwa_ref, ids_ref, route_ref, own_ref, past_ref, terms_ref, base_ref):
        slots = assigned_slots(ids_ref[...], experts, tok_rows)
        route = route_ref[...]
        total = sum(route[place : place + 1, :] for place in range(len(slots)))
        shares = [dwa_ref[depth] * (route[place : place + 1, :] / total) for place in range(len(slots))]
        rest = placed(slots, shares, capacity, tok_rows)
        for place in range(TERMS):
            term = rest.astype(jnp.bfloat16)
            rest = rest - term.astype(jnp.float32)
            terms_ref[place] = term
        base = dwa_ref[depth] * own_ref[...].astype(jnp.float32)
        for layer in range(depth):
            base += dwa_ref[layer] * past_ref[layer].astype(jnp.float32)
        base_ref[...] = base

    shapes = [
        jax.ShapeDtypeStruct((TERMS, experts * height, LANES), jnp.bfloat16),
        jax.ShapeDtypeStruct((tok_rows, features), jnp.float32),
    ]
    operands = (dwa_weight, ids, route, own_columns, past_layers)
    return call(kernel, shapes, *operands, in_specs=[SMEM] + [VMEM] * 4)


def mixed_layers(returned, terms, base, dtype):
    tok_rows, features = base.shape
    experts = returned.shape[0] // RADIX

    def kernel(terms_ref, base_ref, in_ref, out_ref):
        outs = []
        for expert in range(experts):
            total = in_ref[expert * RADIX].astype(jnp.float32)
            for far in range(1, RADIX):
                total += in_ref[expert * RADIX + far].astype(jnp.float32)
            outs.append(total.astype(jnp.bfloat16))
        outs = jnp.concatenate(outs, axis=0)
        mix = jnp.zeros((features // LANES * tok_rows, LANES), jnp.float32)
        for place in range(TERMS):
            mix += lax.dot_general(
                terms_ref[place], outs, (((0,), (0,)), ((), ())), preferred_element_type=jnp.float32
            )
        for block in range(features // LANES):
            lanes = slice(block * LANES, (block + 1) * LANES)
            value = base_ref[:, lanes] + mix[block * tok_rows : (block + 1) * tok_rows]
            out_ref[:, lanes] = value.astype(out_ref.dtype)

    shape = jax.ShapeDtypeStruct((tok_rows, features), dtype)
    return call(kernel, shape, terms, base, returned)


def per_device(
    tokens, expert_ids, route_weight, gate_weight, up_weight, down_weight, past_layers, dwa_weight
):
    experts = lax.axis_size("expert")
    parts = lax.axis_size("tensor")
    tok_rows, feature_width = tokens.shape
    chosen_count = expert_ids.shape[1]
    capacity = min(tok_rows, 3 * chosen_count * tok_rows // (2 * experts))
    quarter = feature_width // parts
    blocks = quarter // LANES
    together = 2 * RADIX
    order = chunk_order(together, capacity, blocks)
    ids = expert_ids.T
    route = jnp.tile(route_weight.T, (1, blocks))
    weights = weights_by_features(gate_weight, up_weight, quarter)
    place = lax.axis_index("tensor").reshape(1)
    packed, own_columns = packed_rows(in_hbm(ids), in_hbm(tokens), place * quarter, quarter, experts, capacity)
    arrived = far_exchange(packed)
    own_set = wide_rows(arrived, jnp.asarray(order, jnp.bfloat16), capacity)
    sets = window_sets(own_set)
    own, *others = gate_up_parts(sets, weights)
    hidden = lax.all_gather(hidden_units(own, tensor_sums(*others)), "tensor", axis=0, tiled=False)
    own, *others = down_sets(hidden, down_weight[0], [jnp.float32] * 2 + [jnp.bfloat16] * 2)
    route, own = lax.optimization_barrier((route, own))
    terms, base = mix_terms(ids, route, own_columns, past_layers, dwa_weight, experts, capacity)
    others = returned_sums(*others)
    own, terms, base = lax.optimization_barrier((own, terms, base))
    returned = far_exchange(summed_chunks(own, others, jnp.asarray(order.T, jnp.bfloat16), capacity))
    return mixed_layers(returned, terms, base, tokens.dtype)


def solution(mesh):
    return jax.shard_map(
        per_device,
        mesh=mesh,
        in_specs=(
            P(("expert", "dp"), None),
            P(("expert", "dp"), None),
            P(("expert", "dp"), None),
            P("expert", None, ("dp", "tensor")),
            P("expert", None, ("dp", "tensor")),
            P("expert", "dp", "tensor"),
            P(None, ("expert", "dp"), "tensor"),
            P(),
        ),
        out_specs=P(("expert", "dp"), "tensor"),
        check_vma=False,
    )
```

```python
import jax
import jax.numpy as jnp
import numpy as np
from jax import lax
from jax.experimental import pallas as pl
from jax.experimental.pallas import tpu as pltpu
from jax.sharding import PartitionSpec as P

RADIX = 4
LANES = 128
TERMS = 3
SHIFTS = (0, 1, 3, 2)
LIMIT = pltpu.CompilerParams(vmem_limit_bytes=16 * 2**20)
HBM = pl.BlockSpec(memory_space=pltpu.HBM)
SMEM = pl.BlockSpec(memory_space=pltpu.SMEM)
VMEM = pl.BlockSpec(memory_space=pltpu.VMEM)


def in_hbm(array):
    return pltpu.with_memory_space_constraint(array, pltpu.HBM)


def far_groups():
    experts, count = lax.axis_size("expert"), lax.axis_size("dp")
    stride = count // RADIX
    return [
        [expert * count + low + stride * high for expert in range(experts) for high in range(RADIX)]
        for low in range(stride)
    ]


def far_exchange(chunks):
    return lax.all_to_all(chunks, ("expert", "dp"), 0, 0, tiled=True, axis_index_groups=far_groups())


def shifted(shard, even_shift, odd_shift):
    experts, count = lax.axis_size("expert"), lax.axis_size("dp")
    pairs = []
    for expert in range(experts):
        shift = odd_shift if expert % 2 else even_shift
        for place in range(count):
            pairs.append((expert * count + place, expert * count + (place + shift) % count))
    return lax.ppermute(shard, ("expert", "dp"), pairs)


def forward(shard):
    return shifted(shard, 1, -1)


def backward(shard):
    return shifted(shard, -1, 1)


def window_sets(own):
    first, other = forward(own), backward(own)
    return [own, first, other, forward(first)]


def returned_sums(first, other, second):
    relayed = backward(second)
    other = forward(other)
    first = (first + relayed.astype(jnp.float32)).astype(jnp.bfloat16)
    return [backward(first), other]


def call(kernel, out_shape, *operands, in_specs=None):
    many = isinstance(out_shape, list)
    return pl.pallas_call(
        kernel,
        out_shape=out_shape,
        in_specs=in_specs or [VMEM] * len(operands),
        out_specs=[VMEM] * len(out_shape) if many else VMEM,
        compiler_params=LIMIT,
    )(*operands)


def repeated_ids(ids):
    tok_rows = ids.shape[1]
    token = lax.broadcasted_iota(jnp.int32, (tok_rows, LANES), 0)
    lane = lax.broadcasted_iota(jnp.int32, (tok_rows, LANES), 1)
    spread = (lane % tok_rows == token).astype(jnp.float32)
    return jnp.dot(ids.astype(jnp.float32), spread, preferred_element_type=jnp.float32)


def earlier_tokens(tok_rows):
    source = lax.broadcasted_iota(jnp.int32, (LANES, LANES), 0)
    token = lax.broadcasted_iota(jnp.int32, (LANES, LANES), 1) % tok_rows
    return (source < token).astype(jnp.float32)


def assigned_slots(ids, experts, before):
    ids = repeated_ids(ids)
    choices, lanes = ids.shape
    expert = lax.broadcasted_iota(jnp.int32, (experts, lanes), 0).astype(jnp.float32)
    chosen = [ids[place : place + 1, :] == expert for place in range(choices)]
    named = sum(mask.astype(jnp.float32) for mask in chosen)
    earlier = jnp.dot(named, before, preferred_element_type=jnp.float32)
    return [jnp.where(mask, earlier, -1.0) for mask in chosen]


def placed(slots, values, capacity, tok_rows):
    experts, lanes = slots[0].shape
    blocks = lanes // tok_rows
    shape = (capacity * blocks, lanes)
    row = lax.broadcasted_iota(jnp.int32, shape, 0)
    column = lax.broadcasted_iota(jnp.int32, shape, 1)
    same_block = row % blocks == column // tok_rows
    slot = (row // blocks).astype(jnp.float32)
    pieces = []
    for expert in range(experts):
        piece = jnp.zeros(shape, jnp.float32)
        for found, value in zip(slots, values):
            piece += jnp.where(same_block & (found[expert : expert + 1, :] == slot), value, 0.0)
        pieces.append(piece)
    return jnp.concatenate(pieces, axis=0)


def packed_rows(ids, tokens, first_column, quarter, experts, capacity):
    tok_rows = tokens.shape[0]
    blocks = quarter // LANES

    def kernel(first_ref, ids_in_ref, tokens_ref, out_ref, own_ref, ids_ref, named, arrived):
        first = pl.multiple_of(first_ref[0], LANES)
        ids_copy = pltpu.make_async_copy(ids_in_ref, ids_ref, named)
        copy = pltpu.make_async_copy(tokens_ref.at[:, pl.ds(first, quarter)], own_ref, arrived)
        ids_copy.start()
        copy.start()
        before = earlier_tokens(tok_rows)
        ids_copy.wait()
        slots = assigned_slots(ids_ref[...], experts, before)
        chosen = placed(slots, [1.0] * len(slots), capacity, tok_rows).astype(jnp.bfloat16)
        copy.wait()
        tall = [own_ref[:, block * LANES : (block + 1) * LANES] for block in range(blocks)]
        out = jnp.dot(chosen, jnp.concatenate(tall, axis=0), preferred_element_type=jnp.float32)
        out = out.astype(out_ref.dtype)
        height = capacity * blocks
        for expert in range(experts):
            for far in range(RADIX):
                out_ref[expert * RADIX + far] = out[expert * height : (expert + 1) * height]

    return pl.pallas_call(
        kernel,
        out_shape=[
            jax.ShapeDtypeStruct((experts * RADIX, capacity * blocks, LANES), tokens.dtype),
            jax.ShapeDtypeStruct((tok_rows, quarter), tokens.dtype),
        ],
        in_specs=[SMEM, HBM, HBM],
        out_specs=[VMEM, VMEM],
        scratch_shapes=[pltpu.VMEM(ids.shape, ids.dtype), pltpu.SemaphoreType.DMA, pltpu.SemaphoreType.DMA],
        compiler_params=LIMIT,
        name="packed_rows",
    )(first_column, ids, tokens)


def chunk_order(chunks, capacity, blocks):
    count = chunks * capacity * blocks
    order = np.arange(count).reshape(chunks, capacity, blocks).transpose(2, 0, 1).reshape(-1)
    return np.eye(count, dtype=np.float32)[order]


def wide_rows(chunks, order, capacity):
    count, height, _ = chunks.shape
    blocks = height // capacity
    together = order.shape[0] // height
    rows = together * capacity

    def kernel(order_ref, in_ref, out_ref):
        for group in range(count // together):
            tall = in_ref[group * together : (group + 1) * together].reshape(together * height, LANES)
            out = jnp.dot(order_ref[...], tall, preferred_element_type=jnp.float32).astype(out_ref.dtype)
            for block in range(blocks):
                piece = out[block * rows : (block + 1) * rows]
                out_ref[group * rows : (group + 1) * rows, block * LANES : (block + 1) * LANES] = piece

    shape = jax.ShapeDtypeStruct((count * capacity, blocks * LANES), chunks.dtype)
    return call(kernel, shape, order, chunks)


def summed_chunks(own, others, order, capacity):
    total_rows, features = own.shape
    blocks = features // LANES
    height = capacity * blocks
    together = order.shape[0] // height
    rows = together * capacity

    def kernel(order_ref, own_ref, *refs):
        other_refs, out_ref = refs[:-1], refs[-1]
        total = own_ref[...]
        for ref in other_refs:
            total += ref[...].astype(jnp.float32)
        total = total.astype(out_ref.dtype)
        for group in range(total_rows // rows):
            part = total[group * rows : (group + 1) * rows]
            tall = [part[:, block * LANES : (block + 1) * LANES] for block in range(blocks)]
            out = jnp.dot(order_ref[...], jnp.concatenate(tall, axis=0), preferred_element_type=jnp.float32)
            out = out.astype(out_ref.dtype).reshape(together, height, LANES)
            out_ref[group * together : (group + 1) * together] = out

    shape = jax.ShapeDtypeStruct((total_rows // capacity, height, LANES), jnp.bfloat16)
    return call(kernel, shape, order, own, *others)


def weights_by_features(gate_weight, up_weight, quarter):
    parts = lax.axis_size("tensor")
    here = lax.axis_index("tensor")
    slabs = [w.reshape(parts, quarter, -1) for w in (gate_weight, up_weight)]

    def slab(shift):
        place = (here + shift) % parts
        both = [lax.dynamic_index_in_dim(w, place, 0, keepdims=False) for w in slabs]
        both = jnp.concatenate(both, axis=1)
        if shift == 0:
            return both
        return lax.ppermute(both, "tensor", [(i, (i + shift) % parts) for i in range(parts)])

    return [slab(shift) for shift in SHIFTS]


def gate_up_parts(sets, weights, place):
    parts = len(weights)
    width = weights[0].shape[1]
    set_rows = sets[0].shape[0]
    rows = set_rows * len(sets)

    def kernel(place_ref, *refs):
        set_refs, w_refs, out_ref = refs[: len(sets)], refs[len(sets) : -1], refs[-1]
        stacked = jnp.concatenate([ref[...] for ref in set_refs], axis=0)
        for shift, w_ref in zip(SHIFTS, w_refs):
            part = (place_ref[0] + (parts - shift)) % parts
            out = jnp.dot(stacked, w_ref[...], preferred_element_type=jnp.float32)
            out_ref[part] = out.astype(out_ref.dtype)

    shape = jax.ShapeDtypeStruct((parts, rows, width), jnp.bfloat16)
    specs = [SMEM] + [VMEM] * (len(sets) + parts)
    return call(kernel, shape, place, *sets, *weights, in_specs=specs)


def hidden_units(parts):
    count, rows, both = parts.shape
    width = both // 2

    def kernel(in_ref, out_ref):
        total = in_ref[0].astype(jnp.float32)
        for part in range(1, count):
            total += in_ref[part].astype(jnp.float32)
        gate, up = total[:, :width], total[:, width:]
        out_ref[...] = (gate / (1.0 + jnp.exp(-gate)) * up).astype(out_ref.dtype)

    return call(kernel, jax.ShapeDtypeStruct((rows, width), jnp.bfloat16), parts)


def down_sets(hidden, w_down, count, places, dtypes):
    parts, rows, _ = hidden.shape
    set_rows = rows // count
    features = w_down.shape[1]

    def kernel(hidden_ref, w_ref, *out_refs):
        taken = slice(places[0] * set_rows, (places[-1] + 1) * set_rows)
        wide = jnp.concatenate([hidden_ref[part, taken, :] for part in range(parts)], axis=1)
        out = jnp.dot(wide, w_ref[...], preferred_element_type=jnp.float32)
        for place, ref in enumerate(out_refs):
            ref[...] = out[place * set_rows : (place + 1) * set_rows].astype(ref.dtype)

    shapes = [jax.ShapeDtypeStruct((set_rows, features), dtype) for dtype in dtypes]
    return call(kernel, shapes, hidden, w_down)


def mix_terms(ids, route, own_columns, past_layers, dwa_weight, experts, capacity):
    tok_rows, features = own_columns.shape
    height = capacity * (features // LANES)
    depth = past_layers.shape[0]

    def kernel(dwa_ref, ids_ref, route_ref, own_ref, past_ref, terms_ref, base_ref):
        slots = assigned_slots(ids_ref[...], experts, earlier_tokens(tok_rows))
        route = route_ref[...]
        total = sum(route[place : place + 1, :] for place in range(len(slots)))
        shares = [dwa_ref[depth] * (route[place : place + 1, :] / total) for place in range(len(slots))]
        rest = placed(slots, shares, capacity, tok_rows)
        for place in range(TERMS):
            term = rest.astype(jnp.bfloat16)
            rest = rest - term.astype(jnp.float32)
            terms_ref[place] = term
        base = dwa_ref[depth] * own_ref[...].astype(jnp.float32)
        for layer in range(depth):
            base += dwa_ref[layer] * past_ref[layer].astype(jnp.float32)
        base_ref[...] = base

    shapes = [
        jax.ShapeDtypeStruct((TERMS, experts * height, LANES), jnp.bfloat16),
        jax.ShapeDtypeStruct((tok_rows, features), jnp.float32),
    ]
    operands = (dwa_weight, ids, route, own_columns, past_layers)
    return call(kernel, shapes, *operands, in_specs=[SMEM] + [VMEM] * 4)


def mixed_layers(returned, terms, base, dtype):
    tok_rows, features = base.shape
    experts = returned.shape[0] // RADIX

    def kernel(terms_ref, base_ref, in_ref, out_ref):
        outs = []
        for expert in range(experts):
            total = in_ref[expert * RADIX].astype(jnp.float32)
            for far in range(1, RADIX):
                total += in_ref[expert * RADIX + far].astype(jnp.float32)
            outs.append(total.astype(jnp.bfloat16))
        outs = jnp.concatenate(outs, axis=0)
        mix = jnp.zeros((features // LANES * tok_rows, LANES), jnp.float32)
        for place in range(TERMS):
            mix += lax.dot_general(
                terms_ref[place], outs, (((0,), (0,)), ((), ())), preferred_element_type=jnp.float32
            )
        for block in range(features // LANES):
            lanes = slice(block * LANES, (block + 1) * LANES)
            value = base_ref[:, lanes] + mix[block * tok_rows : (block + 1) * tok_rows]
            out_ref[:, lanes] = value.astype(out_ref.dtype)

    shape = jax.ShapeDtypeStruct((tok_rows, features), dtype)
    return call(kernel, shape, terms, base, returned)


def per_device(
    tokens, expert_ids, route_weight, gate_weight, up_weight, down_weight, past_layers, dwa_weight
):
    experts = lax.axis_size("expert")
    parts = lax.axis_size("tensor")
    tok_rows, feature_width = tokens.shape
    chosen_count = expert_ids.shape[1]
    capacity = min(tok_rows, 3 * chosen_count * tok_rows // (2 * experts))
    quarter = feature_width // parts
    blocks = quarter // LANES
    together = 2 * RADIX
    order = chunk_order(together, capacity, blocks)
    ids = expert_ids.T
    route = jnp.tile(route_weight.T, (1, blocks))
    weights = weights_by_features(gate_weight, up_weight, quarter)
    place = lax.axis_index("tensor").reshape(1)
    packed, own_columns = packed_rows(in_hbm(ids), in_hbm(tokens), place * quarter, quarter, experts, capacity)
    arrived = far_exchange(packed)
    own_set = wide_rows(arrived, jnp.asarray(order, jnp.bfloat16), capacity)
    sets = window_sets(own_set)
    partial = lax.all_to_all(gate_up_parts(sets, weights, place), "tensor", 0, 0, tiled=True)
    hidden = lax.all_gather(hidden_units(partial), "tensor", axis=0, tiled=False)
    count = len(sets)
    other, second = down_sets(hidden, down_weight[0], count, range(2, count), [jnp.bfloat16] * 2)
    hidden, other, second = lax.optimization_barrier((hidden, other, second))
    own, first = down_sets(hidden, down_weight[0], count, range(2), [jnp.float32] * 2)
    route, own = lax.optimization_barrier((route, own))
    terms, base = mix_terms(ids, route, own_columns, past_layers, dwa_weight, experts, capacity)
    others = returned_sums(first, other, second)
    own, terms, base = lax.optimization_barrier((own, terms, base))
    returned = far_exchange(summed_chunks(own, others, jnp.asarray(order.T, jnp.bfloat16), capacity))
    return mixed_layers(returned, terms, base, tokens.dtype)


def solution(mesh):
    return jax.shard_map(
        per_device,
        mesh=mesh,
        in_specs=(
            P(("expert", "dp"), None),
            P(("expert", "dp"), None),
            P(("expert", "dp"), None),
            P("expert", None, ("dp", "tensor")),
            P("expert", None, ("dp", "tensor")),
            P("expert", "dp", "tensor"),
            P(None, ("expert", "dp"), "tensor"),
            P(),
        ),
        out_specs=P(("expert", "dp"), "tensor"),
        check_vma=False,
    )
```

```python
import jax
import jax.numpy as jnp
import numpy as np
from jax import lax
from jax.experimental import pallas as pl
from jax.experimental.pallas import tpu as pltpu
from jax.sharding import PartitionSpec as P

RADIX = 4
LANES = 128
TERMS = 3
LIMIT = pltpu.CompilerParams(vmem_limit_bytes=16 * 2**20)
HBM = pl.BlockSpec(memory_space=pltpu.HBM)
SMEM = pl.BlockSpec(memory_space=pltpu.SMEM)
VMEM = pl.BlockSpec(memory_space=pltpu.VMEM)


def in_hbm(array):
    return pltpu.with_memory_space_constraint(array, pltpu.HBM)


def far_groups():
    experts, count = lax.axis_size("expert"), lax.axis_size("dp")
    stride = count // RADIX
    return [
        [expert * count + low + stride * high for expert in range(experts) for high in range(RADIX)]
        for low in range(stride)
    ]


def far_exchange(chunks):
    return lax.all_to_all(chunks, ("expert", "dp"), 0, 0, tiled=True, axis_index_groups=far_groups())


def shifted(shard, even_shift, odd_shift):
    experts, count = lax.axis_size("expert"), lax.axis_size("dp")
    pairs = []
    for expert in range(experts):
        shift = odd_shift if expert % 2 else even_shift
        for place in range(count):
            pairs.append((expert * count + place, expert * count + (place + shift) % count))
    return lax.ppermute(shard, ("expert", "dp"), pairs)


def forward(shard):
    return shifted(shard, 1, -1)


def backward(shard):
    return shifted(shard, -1, 1)


def window_sets(own):
    first, other = forward(own), backward(own)
    return [own, first, other, forward(first)]


def returned_sums(first, other, second):
    relayed = backward(second)
    other = forward(other)
    first = (first + relayed.astype(jnp.float32)).astype(jnp.bfloat16)
    return [backward(first), other]


def call(kernel, out_shape, *operands, in_specs=None):
    many = isinstance(out_shape, list)
    return pl.pallas_call(
        kernel,
        out_shape=out_shape,
        in_specs=in_specs or [VMEM] * len(operands),
        out_specs=[VMEM] * len(out_shape) if many else VMEM,
        compiler_params=LIMIT,
    )(*operands)


def repeated_ids(ids):
    tok_rows = ids.shape[1]
    token = lax.broadcasted_iota(jnp.int32, (tok_rows, LANES), 0)
    lane = lax.broadcasted_iota(jnp.int32, (tok_rows, LANES), 1)
    spread = (lane % tok_rows == token).astype(jnp.float32)
    return jnp.dot(ids.astype(jnp.float32), spread, preferred_element_type=jnp.float32)


def earlier_tokens(tok_rows):
    source = lax.broadcasted_iota(jnp.int32, (LANES, LANES), 0)
    token = lax.broadcasted_iota(jnp.int32, (LANES, LANES), 1) % tok_rows
    return (source < token).astype(jnp.float32)


def assigned_slots(ids, experts, before):
    ids = repeated_ids(ids)
    choices, lanes = ids.shape
    expert = lax.broadcasted_iota(jnp.int32, (experts, lanes), 0).astype(jnp.float32)
    chosen = [ids[place : place + 1, :] == expert for place in range(choices)]
    named = sum(mask.astype(jnp.float32) for mask in chosen)
    earlier = jnp.dot(named, before, preferred_element_type=jnp.float32)
    return [jnp.where(mask, earlier, -1.0) for mask in chosen]


def placed(slots, values, capacity, tok_rows):
    experts, lanes = slots[0].shape
    blocks = lanes // tok_rows
    shape = (capacity * blocks, lanes)
    row = lax.broadcasted_iota(jnp.int32, shape, 0)
    column = lax.broadcasted_iota(jnp.int32, shape, 1)
    same_block = row % blocks == column // tok_rows
    slot = (row // blocks).astype(jnp.float32)
    pieces = []
    for expert in range(experts):
        piece = jnp.zeros(shape, jnp.float32)
        for found, value in zip(slots, values):
            piece += jnp.where(same_block & (found[expert : expert + 1, :] == slot), value, 0.0)
        pieces.append(piece)
    return jnp.concatenate(pieces, axis=0)


def packed_rows(ids, tokens, first_column, quarter, experts, capacity):
    tok_rows = tokens.shape[0]
    blocks = quarter // LANES

    def kernel(first_ref, ids_in_ref, tokens_ref, out_ref, own_ref, ids_ref, named, arrived):
        first = pl.multiple_of(first_ref[0], LANES)
        ids_copy = pltpu.make_async_copy(ids_in_ref, ids_ref, named)
        copy = pltpu.make_async_copy(tokens_ref.at[:, pl.ds(first, quarter)], own_ref, arrived)
        ids_copy.start()
        copy.start()
        before = earlier_tokens(tok_rows)
        ids_copy.wait()
        slots = assigned_slots(ids_ref[...], experts, before)
        chosen = placed(slots, [1.0] * len(slots), capacity, tok_rows).astype(jnp.bfloat16)
        copy.wait()
        tall = [own_ref[:, block * LANES : (block + 1) * LANES] for block in range(blocks)]
        out = jnp.dot(chosen, jnp.concatenate(tall, axis=0), preferred_element_type=jnp.float32)
        out = out.astype(out_ref.dtype)
        height = capacity * blocks
        for expert in range(experts):
            for far in range(RADIX):
                out_ref[expert * RADIX + far] = out[expert * height : (expert + 1) * height]

    return pl.pallas_call(
        kernel,
        out_shape=[
            jax.ShapeDtypeStruct((experts * RADIX, capacity * blocks, LANES), tokens.dtype),
            jax.ShapeDtypeStruct((tok_rows, quarter), tokens.dtype),
        ],
        in_specs=[SMEM, HBM, HBM],
        out_specs=[VMEM, VMEM],
        scratch_shapes=[pltpu.VMEM(ids.shape, ids.dtype), pltpu.SemaphoreType.DMA, pltpu.SemaphoreType.DMA],
        compiler_params=LIMIT,
        name="packed_rows",
    )(first_column, ids, tokens)


def chunk_order(chunks, capacity, blocks):
    count = chunks * capacity * blocks
    order = np.arange(count).reshape(chunks, capacity, blocks).transpose(2, 0, 1).reshape(-1)
    return np.eye(count, dtype=np.float32)[order]


def wide_rows(chunks, order, capacity):
    count, height, _ = chunks.shape
    blocks = height // capacity
    together = order.shape[0] // height
    rows = together * capacity

    def kernel(order_ref, in_ref, out_ref):
        for group in range(count // together):
            tall = in_ref[group * together : (group + 1) * together].reshape(together * height, LANES)
            out = jnp.dot(order_ref[...], tall, preferred_element_type=jnp.float32).astype(out_ref.dtype)
            for block in range(blocks):
                piece = out[block * rows : (block + 1) * rows]
                out_ref[group * rows : (group + 1) * rows, block * LANES : (block + 1) * LANES] = piece

    shape = jax.ShapeDtypeStruct((count * capacity, blocks * LANES), chunks.dtype)
    return call(kernel, shape, order, chunks)


def summed_chunks(own, others, order, capacity):
    total_rows, features = own.shape
    blocks = features // LANES
    height = capacity * blocks
    together = order.shape[0] // height
    rows = together * capacity

    def kernel(order_ref, own_ref, *refs):
        other_refs, out_ref = refs[:-1], refs[-1]
        total = own_ref[...]
        for ref in other_refs:
            total += ref[...].astype(jnp.float32)
        total = total.astype(out_ref.dtype)
        for group in range(total_rows // rows):
            part = total[group * rows : (group + 1) * rows]
            tall = [part[:, block * LANES : (block + 1) * LANES] for block in range(blocks)]
            out = jnp.dot(order_ref[...], jnp.concatenate(tall, axis=0), preferred_element_type=jnp.float32)
            out = out.astype(out_ref.dtype).reshape(together, height, LANES)
            out_ref[group * together : (group + 1) * together] = out

    shape = jax.ShapeDtypeStruct((total_rows // capacity, height, LANES), jnp.bfloat16)
    return call(kernel, shape, order, own, *others)


def along_tensor(shard, even_shift, odd_shift):
    experts, count = lax.axis_size("expert"), lax.axis_size("tensor")
    pairs = []
    for expert in range(experts):
        shift = odd_shift if expert % 2 else even_shift
        for place in range(count):
            pairs.append((expert * count + place, expert * count + (place + shift) % count))
    return lax.ppermute(shard, ("expert", "tensor"), pairs)


def weights_by_features(gate_weight, up_weight, quarter):
    parts = lax.axis_size("tensor")
    here = lax.axis_index("tensor")
    step = jnp.where(lax.axis_index("expert") % 2 == 0, 1, parts - 1)
    slabs = [w.reshape(parts, quarter, -1) for w in (gate_weight, up_weight)]

    def slab(shift):
        place = (here + shift) % parts
        both = [lax.dynamic_index_in_dim(w, place, 0, keepdims=False) for w in slabs]
        return jnp.concatenate(both, axis=1)

    moves = [(parts - step, -1, 1), (step, 1, -1), (parts // 2, 2, 2)]
    weights = [slab(0)]
    for shift, even, odd in moves:
        weights.append(along_tensor(slab(shift), even, odd))
    return weights


def gate_up_parts(sets, weights, dtypes):
    width = weights[0].shape[1]
    set_rows = sets[0].shape[0]
    rows = set_rows * len(sets)

    def kernel(*refs):
        set_refs, refs = refs[: len(sets)], refs[len(sets) :]
        w_refs, out_refs = refs[: len(weights)], refs[len(weights) :]
        stacked = jnp.concatenate([ref[...] for ref in set_refs], axis=0)
        for w_ref, out_ref in zip(w_refs, out_refs):
            out = jnp.dot(stacked, w_ref[...], preferred_element_type=jnp.float32)
            out_ref[...] = out.astype(out_ref.dtype)

    shapes = [jax.ShapeDtypeStruct((rows, width), dtype) for dtype in dtypes]
    return call(kernel, shapes, *sets, *weights)


def tensor_sums(following, previous, opposite):
    relayed = along_tensor(opposite, 1, -1)
    previous = along_tensor(previous, -1, 1)
    following = (following + relayed.astype(jnp.float32)).astype(jnp.bfloat16)
    return [along_tensor(following, 1, -1), previous]


def hidden_units(own, others):
    rows, both = own.shape
    width = both // 2

    def kernel(own_ref, *refs):
        other_refs, out_ref = refs[:-1], refs[-1]
        total = own_ref[...]
        for ref in other_refs:
            total += ref[...].astype(jnp.float32)
        gate, up = total[:, :width], total[:, width:]
        out_ref[...] = (gate / (1.0 + jnp.exp(-gate)) * up).astype(out_ref.dtype)

    shape = jax.ShapeDtypeStruct((rows, width), jnp.bfloat16)
    return call(kernel, shape, own, *others)


def down_sets(hidden, w_down, count, places, dtypes):
    parts, rows, _ = hidden.shape
    set_rows = rows // count
    features = w_down.shape[1]

    def kernel(hidden_ref, w_ref, *out_refs):
        taken = slice(places[0] * set_rows, (places[-1] + 1) * set_rows)
        wide = jnp.concatenate([hidden_ref[part, taken, :] for part in range(parts)], axis=1)
        out = jnp.dot(wide, w_ref[...], preferred_element_type=jnp.float32)
        for place, ref in enumerate(out_refs):
            ref[...] = out[place * set_rows : (place + 1) * set_rows].astype(ref.dtype)

    shapes = [jax.ShapeDtypeStruct((set_rows, features), dtype) for dtype in dtypes]
    return call(kernel, shapes, hidden, w_down)


def mix_terms(ids, route, own_columns, past_layers, dwa_weight, experts, capacity):
    tok_rows, features = own_columns.shape
    height = capacity * (features // LANES)
    depth = past_layers.shape[0]

    def kernel(dwa_ref, ids_ref, route_ref, own_ref, past_ref, terms_ref, base_ref):
        slots = assigned_slots(ids_ref[...], experts, earlier_tokens(tok_rows))
        route = route_ref[...]
        total = sum(route[place : place + 1, :] for place in range(len(slots)))
        shares = [dwa_ref[depth] * (route[place : place + 1, :] / total) for place in range(len(slots))]
        rest = placed(slots, shares, capacity, tok_rows)
        for place in range(TERMS):
            term = rest.astype(jnp.bfloat16)
            rest = rest - term.astype(jnp.float32)
            terms_ref[place] = term
        base = dwa_ref[depth] * own_ref[...].astype(jnp.float32)
        for layer in range(depth):
            base += dwa_ref[layer] * past_ref[layer].astype(jnp.float32)
        base_ref[...] = base

    shapes = [
        jax.ShapeDtypeStruct((TERMS, experts * height, LANES), jnp.bfloat16),
        jax.ShapeDtypeStruct((tok_rows, features), jnp.float32),
    ]
    operands = (dwa_weight, ids, route, own_columns, past_layers)
    return call(kernel, shapes, *operands, in_specs=[SMEM] + [VMEM] * 4)


def mixed_layers(returned, terms, base, dtype):
    tok_rows, features = base.shape
    experts = returned.shape[0] // RADIX

    def kernel(terms_ref, base_ref, in_ref, out_ref):
        outs = []
        for expert in range(experts):
            total = in_ref[expert * RADIX].astype(jnp.float32)
            for far in range(1, RADIX):
                total += in_ref[expert * RADIX + far].astype(jnp.float32)
            outs.append(total.astype(jnp.bfloat16))
        outs = jnp.concatenate(outs, axis=0)
        mix = jnp.zeros((features // LANES * tok_rows, LANES), jnp.float32)
        for place in range(TERMS):
            mix += lax.dot_general(
                terms_ref[place], outs, (((0,), (0,)), ((), ())), preferred_element_type=jnp.float32
            )
        for block in range(features // LANES):
            lanes = slice(block * LANES, (block + 1) * LANES)
            value = base_ref[:, lanes] + mix[block * tok_rows : (block + 1) * tok_rows]
            out_ref[:, lanes] = value.astype(out_ref.dtype)

    shape = jax.ShapeDtypeStruct((tok_rows, features), dtype)
    return call(kernel, shape, terms, base, returned)


def per_device(
    tokens, expert_ids, route_weight, gate_weight, up_weight, down_weight, past_layers, dwa_weight
):
    experts = lax.axis_size("expert")
    parts = lax.axis_size("tensor")
    tok_rows, feature_width = tokens.shape
    chosen_count = expert_ids.shape[1]
    capacity = min(tok_rows, 3 * chosen_count * tok_rows // (2 * experts))
    quarter = feature_width // parts
    blocks = quarter // LANES
    together = 2 * RADIX
    order = chunk_order(together, capacity, blocks)
    ids = expert_ids.T
    route = jnp.tile(route_weight.T, (1, blocks))
    weights = weights_by_features(gate_weight, up_weight, quarter)
    place = lax.axis_index("tensor").reshape(1)
    packed, own_columns = packed_rows(in_hbm(ids), in_hbm(tokens), place * quarter, quarter, experts, capacity)
    arrived = far_exchange(packed)
    own_set = wide_rows(arrived, jnp.asarray(order, jnp.bfloat16), capacity)
    sets = window_sets(own_set)
    *weights, far_weights = weights
    (opposite,) = gate_up_parts(sets, [far_weights], [jnp.bfloat16])
    sets, opposite = lax.optimization_barrier((sets, opposite))
    own, following, previous = gate_up_parts(sets, weights, [jnp.float32] * 2 + [jnp.bfloat16])
    units = hidden_units(own, tensor_sums(following, previous, opposite))
    hidden = lax.all_gather(units, "tensor", axis=0, tiled=False)
    count = len(sets)
    other, second = down_sets(hidden, down_weight[0], count, range(2, count), [jnp.bfloat16] * 2)
    hidden, other, second = lax.optimization_barrier((hidden, other, second))
    own, first = down_sets(hidden, down_weight[0], count, range(2), [jnp.float32] * 2)
    route, own = lax.optimization_barrier((route, own))
    terms, base = mix_terms(ids, route, own_columns, past_layers, dwa_weight, experts, capacity)
    others = returned_sums(first, other, second)
    own, terms, base = lax.optimization_barrier((own, terms, base))
    returned = far_exchange(summed_chunks(own, others, jnp.asarray(order.T, jnp.bfloat16), capacity))
    return mixed_layers(returned, terms, base, tokens.dtype)


def solution(mesh):
    return jax.shard_map(
        per_device,
        mesh=mesh,
        in_specs=(
            P(("expert", "dp"), None),
            P(("expert", "dp"), None),
            P(("expert", "dp"), None),
            P("expert", None, ("dp", "tensor")),
            P("expert", None, ("dp", "tensor")),
            P("expert", "dp", "tensor"),
            P(None, ("expert", "dp"), "tensor"),
            P(),
        ),
        out_specs=P(("expert", "dp"), "tensor"),
        check_vma=False,
    )
```
